16 devices in a mesh: dp: 2 (over z), ep: 8 (over y, x, core).
Axes of the slice: x: 2, y: 2, z: 2, core: 2. Of those that a mesh axis runs over, the one named last changes fastest.
Arguments:
- x_in: bfloat16 [2048, 2304], P(('dp', 'ep')), parts along dimension 0
- topk_idx: int32 [2048, 2], P(('dp', 'ep')), parts along dimension 0
- topk_w: float32 [2048, 2], P(('dp', 'ep')), parts along dimension 0
- w_up: bfloat16 [8, 2304, 5760], P('ep')
- w_down: bfloat16 [8, 5760, 2304], P('ep')
Outputs:
- output: bfloat16 [2048, 2304], P(('dp', 'ep')), parts along dimension 0
There are 2 independent parts. The reference program is written for one: setup_inputs(seed, part) draws one part's arguments, and reference() takes and returns one part's arrays. A program takes and returns all parts, laid end to end along the dimension named above; an argument that names none is the same for every part.
All inputs are finite; a program needn't handle non-finite values.
Results may differ from the reference program's by a relative error of at most 0.001.
Values are sent between devices in bfloat16 or wider.
A program may use at most 1 GiB of HBM per device.

```python
import jax
import jax.numpy as jnp
from jax import lax

TOK_DEV = 128
GROUP_SIZE = 8
D_MODEL = 2304
D_FF = 5760
EXPERTS = 8
TOP_K = 2
TOKENS = TOK_DEV * GROUP_SIZE
PAIRS = TOKENS * TOP_K
ROW_WINDOW = min(64, TOKENS)


def draw_routing(route_key):
    key_perm, key_rank, key_start, key_roll = jax.random.split(route_key, 4)
    expert_order = jax.random.permutation(key_perm, EXPERTS).astype(jnp.int32)
    hot_pair = expert_order[:2]
    cold_cycle = expert_order[2:]
    cold_count = EXPERTS - 2
    ranks = jax.vmap(lambda one_key: jax.random.permutation(one_key, TOK_DEV))(jax.random.split(key_rank, GROUP_SIZE)).astype(jnp.int32)
    device_index = jnp.arange(GROUP_SIZE, dtype=jnp.int32)[:, None]
    cold_start = jax.random.randint(key_start, (), 0, cold_count, dtype=jnp.int32)
    cold_base = cold_start + (device_index * TOK_DEV + ranks) * (TOP_K - 1)
    cold_steps = jnp.arange(TOP_K - 1, dtype=jnp.int32)
    cold_ids = cold_cycle[(cold_base[:, :, None] + cold_steps) % cold_count]
    hot_ids = hot_pair[ranks % 2]
    picks = jnp.concatenate([hot_ids[:, :, None], cold_ids], axis=2).reshape(TOKENS, TOP_K)
    shifts = jax.random.randint(key_roll, (TOKENS, 1), 0, TOP_K, dtype=jnp.int32)
    slot_order = (jnp.arange(TOP_K, dtype=jnp.int32)[None, :] + shifts) % TOP_K
    return jnp.take_along_axis(picks, slot_order, axis=1)


def setup_inputs(seed: int = 0, part: int = 0) -> dict:
    part_key = jax.random.fold_in(jax.random.key(seed), part)
    key_x, key_route, key_gate = jax.random.split(part_key, 3)
    key_up, key_down = jax.random.split(jax.random.key(seed + 7919), 2)
    x_in = jax.random.normal(key_x, (TOKENS, D_MODEL), jnp.float32).astype(jnp.bfloat16)
    topk_idx = draw_routing(key_route)
    topk_w = jax.random.uniform(key_gate, (TOKENS, TOP_K), jnp.float32, 0.2, 1.0)
    w_up = lax.map(lambda one_key: (jax.random.normal(one_key, (D_MODEL, D_FF), jnp.float32) * D_MODEL ** -0.5).astype(jnp.bfloat16), jax.random.split(key_up, EXPERTS))
    w_down = lax.map(lambda one_key: (jax.random.normal(one_key, (D_FF, D_MODEL), jnp.float32) * D_FF ** -0.5).astype(jnp.bfloat16), jax.random.split(key_down, EXPERTS))
    return {'x_in': x_in, 'topk_idx': topk_idx, 'topk_w': topk_w, 'w_up': w_up, 'w_down': w_down}


def reference(x_in, topk_idx, topk_w, w_up, w_down):
    flat_ids = topk_idx.reshape(PAIRS)
    order = jnp.argsort(flat_ids, stable=True)
    pad_rows = jnp.zeros((ROW_WINDOW, D_MODEL), x_in.dtype)
    sorted_rows = jnp.concatenate([x_in[order // TOP_K], pad_rows], axis=0)
    counts = jnp.bincount(flat_ids, length=EXPERTS)
    starts = jnp.cumsum(counts) - counts

    def expert_step(expert, results):
        up_mat = w_up[expert]
        down_mat = w_down[expert]

        def window_step(window, acc_rows):
            base = starts[expert] + window * ROW_WINDOW
            rows = lax.dynamic_slice(sorted_rows, (base, 0), (ROW_WINDOW, D_MODEL))
            hidden = jax.nn.gelu(jnp.dot(rows, up_mat, preferred_element_type=jnp.float32), approximate=True).astype(jnp.bfloat16)
            result = jnp.dot(hidden, down_mat, preferred_element_type=jnp.float32).astype(jnp.bfloat16)
            valid = window * ROW_WINDOW + jnp.arange(ROW_WINDOW) < counts[expert]
            current = lax.dynamic_slice(acc_rows, (base, 0), (ROW_WINDOW, D_MODEL))
            return lax.dynamic_update_slice(acc_rows, jnp.where(valid[:, None], result, current), (base, 0))

        windows = (counts[expert] + ROW_WINDOW - 1) // ROW_WINDOW
        return lax.fori_loop(0, windows, window_step, results)

    results = jnp.zeros((PAIRS + ROW_WINDOW, D_MODEL), x_in.dtype)
    results = lax.fori_loop(0, EXPERTS, expert_step, results)
    pair_out = results[jnp.argsort(order)].reshape(TOKENS, TOP_K, D_MODEL)
    mixed = jnp.sum(topk_w[:, :, None] * pair_out.astype(jnp.float32), axis=1)
    return mixed.astype(jnp.bfloat16)
```

```python
import functools

import jax
import jax.numpy as jnp
from jax import lax
from jax.experimental import pallas as pl
from jax.experimental.pallas import tpu as pltpu
from jax.sharding import PartitionSpec as P

MESH = pl.DeviceIdType.MESH
TOK = 128
CAP = 64
EXP = 8
D = 2304
F = 5760
NU = 1024
U_FULL = F // NU
U_REM = F - U_FULL * NU
CW = 1152
NC = D // CW
OWN2_TILE = 2
RELAY_TILE = 4


def remote(src, dst, send_sem, recv_sem, dev):
    return pltpu.make_async_remote_copy(src_ref=src, dst_ref=dst, send_sem=send_sem, recv_sem=recv_sem, device_id={'ep': dev}, device_id_type=MESH)


def moe_kernel(x_hbm, ids_ref, gates_ref, wu_hbm, wd_hbm, y_hbm, wu, wd, xg, back, hid, xs, posg, post, sx, rx, sm, rm, sb, rb, sw, sl):
    me = lax.axis_index('ep')
    c = lax.rem(me, 2)
    x = lax.rem(me // 2, 2)
    y = me // 4

    def dev(yy, xx, cc):
        return yy * 4 + xx * 2 + cc

    partner = dev(y, x, 1 - c)
    first = dev(lax.rem(y + c, 2), lax.rem(x + 1 - c, 2), c)
    second = dev(lax.rem(y + 1 - c, 2), lax.rem(x + c, 2), c)
    others = [dev(lax.rem(y + dy, 2), lax.rem(x + dx, 2), lax.rem(c + dc, 2)) for dy, dx, dc in ((0, 0, 1), (0, 1, 0), (1, 0, 0), (0, 1, 1), (1, 0, 1), (1, 1, 0), (1, 1, 1))]

    def source(i, cc):
        lo, hi = lax.rem(i, 2), i // 2
        fx = lo * (1 - cc) + hi * cc
        fy = hi * (1 - cc) + lo * cc
        return dev(lax.rem(y + fy, 2), lax.rem(x + fx, 2), cc)

    own_load = pltpu.make_async_copy(x_hbm, xg.at[me], sl.at[0])
    own_load.start()

    def up_load(t):
        cols = pl.ds(pl.multiple_of(t * NU, 128), NU)
        return pltpu.make_async_copy(wu_hbm.at[0, :, cols], wu.at[:, cols], sw.at[t])

    def up_rem_load():
        cols = pl.ds(U_FULL * NU, U_REM)
        return pltpu.make_async_copy(wu_hbm.at[0, :, cols], wu.at[:, cols], sw.at[U_FULL])

    def down_load(n):
        cols = pl.ds(pl.multiple_of(n * CW, 128), CW)
        return pltpu.make_async_copy(wd_hbm.at[0, :, cols], wd.at[:, cols], sw.at[U_FULL + 1 + n])

    for t in range(U_FULL):
        up_load(t).start()
    up_rem_load().start()
    for n in range(NC):
        down_load(n).start()

    barrier = pltpu.get_barrier_semaphore()
    for other in others:
        pl.semaphore_signal(barrier, inc=1, device_id={'ep': other}, device_id_type=MESH)

    lane = lax.broadcasted_iota(jnp.int32, (TOK, TOK), 1)
    row = lax.broadcasted_iota(jnp.int32, (TOK, TOK), 0)
    id0 = ids_ref[:, 0:1]
    id1 = ids_ref[:, 1:2]
    hit = (id0 == lane) | (id1 == lane)
    lower = jnp.where(lane < row, 1.0, 0.0).astype(jnp.bfloat16)
    rank = jnp.dot(lower, jnp.where(hit, 1.0, 0.0).astype(jnp.bfloat16), preferred_element_type=jnp.float32)
    slot = jnp.where(hit, rank, -1.0)
    post[...] = slot
    posg[me] = slot.T[0:EXP]

    pl.semaphore_wait(barrier, EXP - 1)
    own_load.wait()

    own_first = remote(xg.at[me], xg.at[me], sx.at[0], rx.at[me], first)
    own_partner = remote(xg.at[me], xg.at[me], sx.at[1], rx.at[me], partner)
    own_second = remote(xg.at[me], xg.at[me], sx.at[2], rx.at[me], second)
    metas = [remote(posg.at[me], posg.at[me], sm.at[k], rm.at[me], other) for k, other in enumerate(others)]

    def arrived(s):
        return remote(xg.at[s], xg.at[s], sx.at[0], rx.at[s], partner)

    def meta_arrived(s):
        return remote(posg.at[s], posg.at[s], sm.at[0], rm.at[s], partner)

    def relay(i):
        s = source(i, c)
        return remote(xg.at[s], xg.at[s], sx.at[3 + i], rx.at[s], partner)

    def forward():
        s = source(1, c)
        return remote(xg.at[s], xg.at[s], sx.at[3], rx.at[s], second)

    for meta in metas:
        meta.start()
    own_first.start()
    own_partner.start()

    def up_tile(j, cols):
        z = jnp.dot(xs[...], wu[:, cols], preferred_element_type=jnp.float32)
        hid[jnp.minimum(j, 1), :, cols] = jax.nn.gelu(z, approximate=True).astype(jnp.bfloat16)

    def back_send(i, s, n):
        cols = pl.ds(pl.multiple_of(n * CW, 128), CW)
        return remote(xg.at[source(i, 1 - c), pl.ds(s * CAP, CAP), cols], back.at[me, :, cols], sb.at[(i * 2 + s) * NC + n], rb.at[me, n], source(i, s))

    def back_partner(n):
        cols = pl.ds(pl.multiple_of(n * CW, 128), CW)
        return remote(xg.at[partner, pl.ds(pl.multiple_of((1 - c) * CAP, CAP), CAP), cols], back.at[me, :, cols], sb.at[n], rb.at[me, n], partner)

    def phase(j, carry):
        @pl.when(j < 4)
        def _up():
            @pl.when(j == 0)
            def _():
                arrived(partner).wait_recv()
                meta_arrived(partner).wait_recv()

            @pl.when(j > 0)
            def _():
                arrived(source(j, 1 - c)).wait_recv()
                meta_arrived(source(j, 0)).wait_recv()
                meta_arrived(source(j, 1)).wait_recv()

            for s in range(2):
                s_id = source(j, s)
                where = posg[s_id, pl.ds(me, 1), :]
                slots = lax.broadcasted_iota(jnp.int32, (CAP, TOK), 0).astype(jnp.float32)
                pick = jnp.where(slots == where, 1.0, 0.0).astype(jnp.bfloat16)
                xs[s * CAP:(s + 1) * CAP, :] = jnp.dot(pick, xg[s_id], preferred_element_type=jnp.float32).astype(jnp.bfloat16)

            def tile(t, carry):
                @pl.when(j == 0)
                def _():
                    up_load(t).wait()

                    @pl.when(t == OWN2_TILE)
                    def _():
                        own_second.start()

                    @pl.when(t == RELAY_TILE)
                    def _():
                        arrived(source(1, c)).wait_recv()
                        relay(1).start()
                        forward().start()

                up_tile(j, pl.ds(pl.multiple_of(t * NU, 128), NU))
                return carry

            lax.fori_loop(0, U_FULL, tile, 0)

            @pl.when(j == 0)
            def _():
                up_rem_load().wait()

            up_tile(j, pl.ds(U_FULL * NU, U_REM))

        @pl.when((j == 1) | (j == 2))
        def _():
            arrived(source(j + 1, c)).wait_recv()
            relay(j + 1).start()

        @pl.when(j > 0)
        def _down():
            i = lax.rem(j, 4)

            def tile(n, carry):
                @pl.when(j == 1)
                def _():
                    down_load(n).wait()

                cols = pl.ds(pl.multiple_of(n * CW, 128), CW)
                o = jnp.dot(hid[jnp.minimum(i, 1)], wd[:, cols], preferred_element_type=jnp.float32).astype(jnp.bfloat16)
                xg[source(i, 1 - c), :, cols] = o

                @pl.when(i > 0)
                def _():
                    back_send(i, 0, n).start()
                    back_send(i, 1, n).start()

                @pl.when(i == 0)
                def _():
                    back_partner(n).start()
                    back[me, :, cols] = xg[partner, pl.ds(pl.multiple_of(c * CAP, CAP), CAP), cols]

                return carry

            lax.fori_loop(0, NC, tile, 0)

        return carry

    lax.fori_loop(0, 5, phase, 0)

    slot = post[...]
    parts = []
    for k in range(EXP // 2):
        low = lane < CAP
        at = jnp.where(low, slot[:, 2 * k:2 * k + 1], slot[:, 2 * k + 1:2 * k + 2])
        parts.append((at.astype(jnp.int32) == lane - jnp.where(low, 0, CAP), 2 * k + jnp.where(low, 0, 1)))
    picks = jnp.concatenate([jnp.concatenate([jnp.where(here & (expert == idj), 1.0, 0.0).astype(jnp.bfloat16) for here, expert in parts], axis=1) for idj in (id0, id1)], axis=0)
    g0 = gates_ref[:, 0:1]
    g1 = gates_ref[:, 1:2]

    def y_store(n):
        cols = pl.ds(n * CW, CW)
        return pltpu.make_async_copy(xs.at[:, cols], y_hbm.at[:, cols], sl.at[1 + n])

    for n in range(NC):
        cols = pl.ds(n * CW, CW)
        for other in others:
            remote(back.at[other, :, cols], back.at[other, :, cols], sb.at[0], rb.at[other, n], partner).wait_recv()
        rows = back[:, :, cols].reshape(EXP * CAP, CW)
        got = jnp.dot(picks, rows, preferred_element_type=jnp.float32)
        xs[:, cols] = (g0 * got[:TOK] + g1 * got[TOK:]).astype(jnp.bfloat16)
        y_store(n).start()

    own_first.wait_send()
    own_partner.wait_send()
    own_second.wait_send()
    forward().wait_send()
    for i in range(1, 4):
        relay(i).wait_send()
    for meta in metas:
        meta.wait_send()
    for n in range(NC):
        back_partner(n).wait_send()
        for i in (1, 2, 3):
            for s in range(2):
                back_send(i, s, n).wait_send()
    for n in range(NC):
        y_store(n).wait()


def solution(mesh):
    token_spec = P(('dp', 'ep'), None)
    expert_spec = P('ep', None, None)
    vmem = pl.BlockSpec(memory_space=pltpu.VMEM)
    anyspace = pl.BlockSpec(memory_space=pl.ANY)
    bf16, f32 = jnp.bfloat16, jnp.float32

    def local_layer(x_loc, ids_loc, gates_loc, w_up, w_down):
        return pl.pallas_call(
            moe_kernel,
            out_shape=jax.ShapeDtypeStruct((TOK, D), bf16),
            in_specs=[anyspace, vmem, vmem, anyspace, anyspace],
            out_specs=anyspace,
            scratch_shapes=[
                pltpu.VMEM((D, F), bf16),
                pltpu.VMEM((F, D), bf16),
                pltpu.VMEM((EXP, TOK, D), bf16),
                pltpu.VMEM((EXP, CAP, D), bf16),
                pltpu.VMEM((2, TOK, F), bf16),
                pltpu.VMEM((TOK, D), bf16),
                pltpu.VMEM((EXP, EXP, TOK), f32),
                pltpu.VMEM((TOK, TOK), f32),
                pltpu.SemaphoreType.DMA((7,)),
                pltpu.SemaphoreType.DMA((EXP,)),
                pltpu.SemaphoreType.DMA((7,)),
                pltpu.SemaphoreType.DMA((EXP,)),
                pltpu.SemaphoreType.DMA((8 * NC,)),
                pltpu.SemaphoreType.DMA((EXP, NC)),
                pltpu.SemaphoreType.DMA((U_FULL + 1 + NC,)),
                pltpu.SemaphoreType.DMA((1 + NC,)),
            ],
            compiler_params=pltpu.CompilerParams(vmem_limit_bytes=67043328, collective_id=0, has_side_effects=True),
        )(x_loc, ids_loc, gates_loc, w_up, w_down)

    return jax.shard_map(local_layer, mesh=mesh, in_specs=(token_spec, token_spec, token_spec, expert_spec, expert_spec), out_specs=token_spec, check_vma=False)
```

```python
import functools

import jax
import jax.numpy as jnp
from jax import lax
from jax.experimental import pallas as pl
from jax.experimental.pallas import tpu as pltpu
from jax.sharding import PartitionSpec as P

MESH = pl.DeviceIdType.MESH
TOK = 128
CAP = 64
EXP = 8
D = 2304
F = 5760
NU = 1024
NT = -(-F // NU)
AHEAD = 4
DOWN = ((0, 1024), (1024, 1280))
MSG = ((0, 512), (512, 512), (1024, 768), (1792, 512))
NM = len(MSG)
SPLIT = 48
VMEM_LIMIT = 67043328


def remote(src, dst, send_sem, recv_sem, dev):
    return pltpu.make_async_remote_copy(src_ref=src, dst_ref=dst, send_sem=send_sem, recv_sem=recv_sem, device_id={'ep': dev}, device_id_type=MESH)


def moe_kernel(x_hbm, ids_ref, gates_ref, wu_hbm, wd_hbm, y_ref, wu, wd, xg, back, hid, xs, posg, post, sx, rx, sm, rm, sb, rb, rz, sw, sl):
    me = lax.axis_index('ep')
    c = lax.rem(me, 2)
    x = lax.rem(me // 2, 2)
    y = me // 4

    def dev(yy, xx, cc):
        return yy * 4 + xx * 2 + cc

    partner = dev(y, x, 1 - c)
    first = dev(lax.rem(y + c, 2), lax.rem(x + 1 - c, 2), c)
    second = dev(lax.rem(y + 1 - c, 2), lax.rem(x + c, 2), c)
    others = [dev(lax.rem(y + dy, 2), lax.rem(x + dx, 2), lax.rem(c + dc, 2)) for dy, dx, dc in ((0, 0, 1), (0, 1, 0), (1, 0, 0), (0, 1, 1), (1, 0, 1), (1, 1, 0), (1, 1, 1))]

    def source(i, cc):
        lo, hi = lax.rem(i, 2), i // 2
        fx = lo * (1 - cc) + hi * cc
        fy = hi * (1 - cc) + lo * cc
        return dev(lax.rem(y + fy, 2), lax.rem(x + fx, 2), cc)

    own_load = pltpu.make_async_copy(x_hbm, xg.at[me], sl.at[0])
    own_load.start()

    def up_cols(t):
        return pl.ds(t * NU, min(NU, F - t * NU))

    def down_cols(n):
        return pl.ds(*DOWN[n])

    def msg_cols(m):
        return pl.ds(*MSG[m])

    def up_load(t):
        return pltpu.make_async_copy(wu_hbm.at[0, :, up_cols(t)], wu.at[:, up_cols(t)], sw.at[t])

    def down_load(n):
        return pltpu.make_async_copy(wd_hbm.at[0, :, down_cols(n)], wd.at[:, down_cols(n)], sw.at[NT + n])

    barrier = pltpu.get_barrier_semaphore()
    for other in others:
        pl.semaphore_signal(barrier, inc=1, device_id={'ep': other}, device_id_type=MESH)

    lane = lax.broadcasted_iota(jnp.int32, (TOK, TOK), 1)
    row = lax.broadcasted_iota(jnp.int32, (TOK, TOK), 0)
    expert_row = lax.broadcasted_iota(jnp.int32, (EXP, TOK), 0)
    hit = (ids_ref[0:1, :] == expert_row) | (ids_ref[1:2, :] == expert_row)
    upper = jnp.where(row < lane, 1.0, 0.0).astype(jnp.bfloat16)
    rank = jnp.dot(jnp.where(hit, 1.0, 0.0).astype(jnp.bfloat16), upper, preferred_element_type=jnp.float32)
    slots = jnp.where(hit, rank, -1.0)
    posg[me] = slots
    pad = jnp.zeros((TOK - EXP - 4, TOK), jnp.float32)
    post[...] = jnp.concatenate([slots, ids_ref[...].astype(jnp.float32), gates_ref[...], pad], axis=0).T

    with jax.named_scope('own_load'):
        own_load.wait()
    for t in range(AHEAD):
        up_load(t).start()
    with jax.named_scope('barrier'):
        pl.semaphore_wait(barrier, EXP - 1)

    own_first = remote(xg.at[me], xg.at[me], sx.at[0], rx.at[me], first)
    own_partner = remote(xg.at[me], xg.at[me], sx.at[1], rx.at[me], partner)
    own_second = [remote(xg.at[me, rows], xg.at[me, rows], sx.at[2 + 5 * p], (rx.at[me], rz)[p], second) for p, rows in enumerate((pl.ds(0, SPLIT), pl.ds(SPLIT, TOK - SPLIT)))]
    metas = [remote(posg.at[me], posg.at[me], sm.at[k], rm.at[me], other) for k, other in enumerate(others)]

    def arrived(s):
        return remote(xg.at[s], xg.at[s], sx.at[0], rx.at[s], partner)

    def meta_arrived(s):
        return remote(posg.at[s], posg.at[s], sm.at[0], rm.at[s], partner)

    def relay(i):
        s = source(i, c)
        return remote(xg.at[s], xg.at[s], sx.at[3 + i], rx.at[s], partner)

    def forward():
        s = source(1, c)
        return remote(xg.at[s], xg.at[s], sx.at[3], rx.at[s], second)

    def back_send(i, s, m):
        return remote(xg.at[source(i, 1 - c), pl.ds(s * CAP, CAP), msg_cols(m)], back.at[me, :, msg_cols(m)], sb.at[(i * 2 + s) * NM + m], rb.at[me, m], source(i, s))

    def back_partner(m):
        return remote(xg.at[partner, pl.ds(pl.multiple_of((1 - c) * CAP, CAP), CAP), msg_cols(m)], back.at[me, :, msg_cols(m)], sb.at[m], rb.at[me, m], partner)

    def gather(i):
        for s in range(2):
            s_id = source(i, s)
            where = posg[s_id, pl.ds(me, 1), :]
            rank_row = lax.broadcasted_iota(jnp.int32, (CAP, TOK), 0).astype(jnp.float32)
            pick = jnp.where(rank_row == where, 1.0, 0.0).astype(jnp.bfloat16)
            xs[s * CAP:(s + 1) * CAP, :] = jnp.dot(pick, xg[s_id], preferred_element_type=jnp.float32).astype(jnp.bfloat16)

    def up_tile(h, t):
        z = jnp.dot(xs[...], wu[:, up_cols(t)], preferred_element_type=jnp.float32)
        hid[h, :, up_cols(t)] = jax.nn.gelu(z, approximate=True).astype(jnp.bfloat16)

    def down_tile(h, i, n):
        xg[source(i, 1 - c), :, down_cols(n)] = jnp.dot(hid[h], wd[:, down_cols(n)], preferred_element_type=jnp.float32).astype(jnp.bfloat16)

    def own_down(n):
        down_tile(0, 0, n)
        for m in (2 * n, 2 * n + 1):
            back_partner(m).start()
        back[me, :, down_cols(n)] = xg[partner, pl.ds(pl.multiple_of(c * CAP, CAP), CAP), down_cols(n)]

    with jax.named_scope('start'):
        for meta in metas:
            meta.start()
        own_first.start()
        own_partner.start()
        for t in range(AHEAD, NT):
            up_load(t).start()
    with jax.named_scope('wait_partner'):
        arrived(partner).wait_recv()
        meta_arrived(partner).wait_recv()
    with jax.named_scope('up0'):
        gather(0)
        for t in range(NT):
            up_load(t).wait()
            if t == AHEAD - 1:
                down_load(0).start()
            if t == NT - 1:
                own_second[0].start()
                down_load(1).start()
            up_tile(0, t)
    with jax.named_scope('wait_f'):
        arrived(source(1, c)).wait_recv()
        relay(1).start()
        forward().start()
        own_second[1].start()
    with jax.named_scope('own_down'):
        down_load(0).wait()
        own_down(0)

    def chunk(k, carry):
        i = jnp.where(k == 1, 1, 5 - k)
        with jax.named_scope('wait_chunk'):
            arrived(source(i, 1 - c)).wait_recv()
            meta_arrived(source(i, 0)).wait_recv()
            meta_arrived(source(i, 1)).wait_recv()
        with jax.named_scope('up'):
            gather(i)
            for t in range(NT):
                up_tile(1, t)

        for n in range(2):
            with jax.named_scope('down'):
                down_tile(1, i, n)
                for m in (2 * n, 2 * n + 1):
                    for s in range(2):
                        back_send(i, s, m).start()
            if n == 0:
                with jax.named_scope('wait_direct'):
                    @pl.when(k == 1)
                    def _():
                        down_load(1).wait()

                    @pl.when(k == 2)
                    def _():
                        remote(xg.at[source(2, c), pl.ds(SPLIT, TOK - SPLIT)], xg.at[source(2, c), pl.ds(SPLIT, TOK - SPLIT)], sx.at[0], rz, partner).wait_recv()
                        remote(xg.at[source(2, c), pl.ds(0, SPLIT)], xg.at[source(2, c), pl.ds(0, SPLIT)], sx.at[0], rx.at[source(2, c)], partner).wait_recv()
                        relay(2).start()

                    @pl.when(k == 1)
                    def _():
                        arrived(source(3, c)).wait_recv()
                        relay(3).start()
        return carry

    lax.fori_loop(1, 4, chunk, 0)
    with jax.named_scope('own_down'):
        own_down(1)

    cols8 = post[...]
    low = lane < CAP
    parts = []
    for k in range(EXP // 2):
        at = jnp.where(low, cols8[:, 2 * k:2 * k + 1], cols8[:, 2 * k + 1:2 * k + 2])
        here = at == (lane - jnp.where(low, 0, CAP)).astype(jnp.float32)
        parts.append((here, (2 * k + jnp.where(low, 0, 1)).astype(jnp.float32)))
    choice = [cols8[:, EXP + j:EXP + j + 1] for j in range(2)]
    picks = jnp.concatenate([jnp.concatenate([jnp.where(here & (expert == idj), 1.0, 0.0).astype(jnp.bfloat16) for here, expert in parts], axis=1) for idj in choice], axis=0)
    g0 = cols8[:, EXP + 2:EXP + 3]
    g1 = cols8[:, EXP + 3:EXP + 4]

    for m in range(NM):
        cols = msg_cols(m)
        with jax.named_scope('wait_back'):
            for other in others:
                remote(back.at[other, :, cols], back.at[other, :, cols], sb.at[0], rb.at[other, m], partner).wait_recv()
        with jax.named_scope('combine'):
            rows = back[:, :, cols].reshape(EXP * CAP, MSG[m][1])
            got = jnp.dot(picks, rows, preferred_element_type=jnp.float32)
            y_ref[:, cols] = (g0 * got[:TOK] + g1 * got[TOK:]).astype(jnp.bfloat16)

    own_first.wait_send()
    own_partner.wait_send()
    for piece in own_second:
        piece.wait_send()
    forward().wait_send()
    for i in range(1, 4):
        relay(i).wait_send()
    for meta in metas:
        meta.wait_send()
    for m in range(NM):
        back_partner(m).wait_send()
        for i in range(1, 4):
            for s in range(2):
                back_send(i, s, m).wait_send()


def solution(mesh):
    token_spec = P(('dp', 'ep'), None)
    expert_spec = P('ep', None, None)
    vmem = pl.BlockSpec(memory_space=pltpu.VMEM)
    anyspace = pl.BlockSpec(memory_space=pl.ANY)
    bf16, f32 = jnp.bfloat16, jnp.float32

    def local_layer(x_loc, ids_loc, gates_loc, w_up, w_down):
        return pl.pallas_call(
            moe_kernel,
            out_shape=jax.ShapeDtypeStruct((TOK, D), bf16),
            in_specs=[anyspace, vmem, vmem, anyspace, anyspace],
            out_specs=vmem,
            scratch_shapes=[
                pltpu.VMEM((D, F), bf16),
                pltpu.VMEM((F, D), bf16),
                pltpu.VMEM((EXP, TOK, D), bf16),
                pltpu.VMEM((EXP, CAP, D), bf16),
                pltpu.VMEM((2, TOK, F), bf16),
                pltpu.VMEM((TOK, D), bf16),
                pltpu.VMEM((EXP, EXP, TOK), f32),
                pltpu.VMEM((TOK, TOK), f32),
                pltpu.SemaphoreType.DMA((8,)),
                pltpu.SemaphoreType.DMA((EXP,)),
                pltpu.SemaphoreType.DMA((7,)),
                pltpu.SemaphoreType.DMA((EXP,)),
                pltpu.SemaphoreType.DMA((8 * NM,)),
                pltpu.SemaphoreType.DMA((EXP, NM)),
                pltpu.SemaphoreType.DMA,
                pltpu.SemaphoreType.DMA((NT + 2,)),
                pltpu.SemaphoreType.DMA((1,)),
            ],
            compiler_params=pltpu.CompilerParams(vmem_limit_bytes=VMEM_LIMIT, collective_id=0, has_side_effects=True),
        )(x_loc, ids_loc.T, gates_loc.T, w_up, w_down)

    return jax.shard_map(local_layer, mesh=mesh, in_specs=(token_spec, token_spec, token_spec, expert_spec, expert_spec), out_specs=token_spec, check_vma=False)
```

```python
import functools

import jax
import jax.numpy as jnp
from jax import lax
from jax.experimental import pallas as pl
from jax.experimental.pallas import tpu as pltpu
from jax.sharding import PartitionSpec as P

MESH = pl.DeviceIdType.MESH
TOK = 128
CAP = 64
EXP = 8
D = 2304
F = 5760
NU = 1024
NT = -(-F // NU)
F_TILE = 4
AHEAD = 2
DOWN = ((0, 1024), (1024, 1280))
MSG = ((0, 512), (512, 512), (1024, 768), (1792, 512))
NM = len(MSG)
HALF = TOK // 2
VMEM_LIMIT = 67043328


def remote(src, dst, send_sem, recv_sem, dev):
    return pltpu.make_async_remote_copy(src_ref=src, dst_ref=dst, send_sem=send_sem, recv_sem=recv_sem, device_id={'ep': dev}, device_id_type=MESH)


def moe_kernel(x_hbm, ids_hbm, gates_hbm, wu_hbm, wd_hbm, y_ref, ids_ref, gates_ref, wu, wd, xg, back, hid, xs, posg, post, sx, rx, sm, rm, sb, rb, sw, sl):
    me = lax.axis_index('ep')
    c = lax.rem(me, 2)
    x = lax.rem(me // 2, 2)
    y = me // 4

    def dev(yy, xx, cc):
        return yy * 4 + xx * 2 + cc

    partner = dev(y, x, 1 - c)
    first = dev(lax.rem(y + c, 2), lax.rem(x + 1 - c, 2), c)
    second = dev(lax.rem(y + 1 - c, 2), lax.rem(x + c, 2), c)
    others = [dev(lax.rem(y + dy, 2), lax.rem(x + dx, 2), lax.rem(c + dc, 2)) for dy, dx, dc in ((0, 0, 1), (0, 1, 0), (1, 0, 0), (0, 1, 1), (1, 0, 1), (1, 1, 0), (1, 1, 1))]

    def source(i, cc):
        lo, hi = lax.rem(i, 2), i // 2
        fx = lo * (1 - cc) + hi * cc
        fy = hi * (1 - cc) + lo * cc
        return dev(lax.rem(y + fy, 2), lax.rem(x + fx, 2), cc)

    barrier = pltpu.get_barrier_semaphore()
    for other in (partner, first, second):
        pl.semaphore_signal(barrier, inc=1, device_id={'ep': other}, device_id_type=MESH)
    ids_load = pltpu.make_async_copy(ids_hbm, ids_ref, sl.at[1])
    gates_load = pltpu.make_async_copy(gates_hbm, gates_ref, sl.at[2])
    ids_load.start()
    gates_load.start()
    own_load = pltpu.make_async_copy(x_hbm, xg.at[me], sl.at[0])
    own_load.start()

    def up_cols(t):
        return pl.ds(t * NU, min(NU, F - t * NU))

    def down_cols(n):
        return pl.ds(*DOWN[n])

    def msg_cols(m):
        return pl.ds(*MSG[m])

    def up_load(t):
        return pltpu.make_async_copy(wu_hbm.at[0, :, up_cols(t)], wu.at[:, up_cols(t)], sw.at[t])

    def down_load(n):
        return pltpu.make_async_copy(wd_hbm.at[0, :, down_cols(n)], wd.at[:, down_cols(n)], sw.at[NT + n])

    ids_load.wait()
    gates_load.wait()
    lane = lax.broadcasted_iota(jnp.int32, (TOK, TOK), 1)
    row = lax.broadcasted_iota(jnp.int32, (TOK, TOK), 0)
    expert_row = lax.broadcasted_iota(jnp.int32, (EXP, TOK), 0)
    hit = (ids_ref[0:1, :] == expert_row) | (ids_ref[1:2, :] == expert_row)
    upper = jnp.where(row < lane, 1.0, 0.0).astype(jnp.bfloat16)
    rank = jnp.dot(jnp.where(hit, 1.0, 0.0).astype(jnp.bfloat16), upper, preferred_element_type=jnp.float32)
    slots = jnp.where(hit, rank, -1.0)
    posg[me] = slots
    pad = jnp.zeros((TOK - EXP - 4, TOK), jnp.float32)
    post[...] = jnp.concatenate([slots, ids_ref[...].astype(jnp.float32), gates_ref[...], pad], axis=0).T

    with jax.named_scope('own_load'):
        own_load.wait()
    for t in range(AHEAD):
        up_load(t).start()
    with jax.named_scope('barrier'):
        pl.semaphore_wait(barrier, 3)

    def block(s, k, p, to):
        rows = pl.ds(p * HALF, HALF)
        return remote(xg.at[s, rows], xg.at[s, rows], sx.at[k, p], rx.at[s, p], to)

    def own(k, p):
        return block(me, k, p, (first, partner, second)[k])

    def forward(p):
        return block(source(1, c), 3, p, second)

    def relay(i, p):
        return block(source(i, c), 3 + i, p, partner)

    def arrived(s, p):
        block(s, 0, p, partner).wait_recv()

    def meta_arrived(s):
        meta(s, 0, partner).wait_recv()

    def meta(s, k, to):
        return remote(posg.at[s], posg.at[s], sm.at[k], rm.at[s], to)

    own_metas = [meta(me, k, to) for k, to in enumerate((first, partner, second))]

    def forward_meta():
        return meta(source(1, c), 3, second)

    def relay_meta(i):
        return meta(source(i, c), 3 + i, partner)

    def back_send(i, s, m):
        return remote(xg.at[source(i, 1 - c), pl.ds(s * CAP, CAP), msg_cols(m)], back.at[me, :, msg_cols(m)], sb.at[(i * 2 + s) * NM + m], rb.at[me, m], source(i, s))

    def back_partner(m):
        return remote(xg.at[partner, pl.ds(pl.multiple_of((1 - c) * CAP, CAP), CAP), msg_cols(m)], back.at[me, :, msg_cols(m)], sb.at[m], rb.at[me, m], partner)

    def gather(i):
        for s in range(2):
            s_id = source(i, s)
            where = posg[s_id, pl.ds(me, 1), :]
            rank_row = lax.broadcasted_iota(jnp.int32, (CAP, TOK), 0).astype(jnp.float32)
            pick = jnp.where(rank_row == where, 1.0, 0.0).astype(jnp.bfloat16)
            xs[s * CAP:(s + 1) * CAP, :] = jnp.dot(pick, xg[s_id], preferred_element_type=jnp.float32).astype(jnp.bfloat16)

    def up_tile(h, t):
        z = jnp.dot(xs[...], wu[:, up_cols(t)], preferred_element_type=jnp.float32)
        hid[h, :, up_cols(t)] = jax.nn.gelu(z, approximate=True).astype(jnp.bfloat16)

    def down_tile(h, i, n):
        xg[source(i, 1 - c), :, down_cols(n)] = jnp.dot(hid[h], wd[:, down_cols(n)], preferred_element_type=jnp.float32).astype(jnp.bfloat16)

    def own_down(n):
        down_tile(0, 0, n)
        for m in (2 * n, 2 * n + 1):
            back_partner(m).start()
        back[me, :, down_cols(n)] = xg[partner, pl.ds(pl.multiple_of(c * CAP, CAP), CAP), down_cols(n)]

    with jax.named_scope('start'):
        for own_meta in own_metas:
            own_meta.start()
        for k in range(2):
            for p in range(2):
                own(k, p).start()
        for t in range(AHEAD, 4):
            up_load(t).start()
    with jax.named_scope('wait_partner'):
        meta_arrived(partner)
        for p in range(2):
            arrived(partner, p)
    with jax.named_scope('up0'):
        gather(0)
        for t in range(NT):
            up_load(t).wait()
            if t < 2:
                up_load(4 + t).start()
            if t == 2:
                down_load(0).start()
            if t == F_TILE:
                with jax.named_scope('wait_f0'):
                    meta_arrived(source(1, c))
                    arrived(source(1, c), 0)
                forward_meta().start()
                forward(0).start()
                relay_meta(1).start()
                relay(1, 0).start()
            if t == NT - 1:
                down_load(1).start()
            up_tile(0, t)
    with jax.named_scope('wait_f1'):
        arrived(source(1, c), 1)
        forward(1).start()
        relay(1, 1).start()
        for p in range(2):
            own(2, p).start()

    def chunk(k, carry):
        i = jnp.where(k == 1, 1, 5 - k)
        with jax.named_scope('wait_chunk'):
            meta_arrived(source(i, 1 - c))
            for p in range(2):
                arrived(source(i, 1 - c), p)
        with jax.named_scope('up'):
            gather(i)
            for t in range(NT):
                up_tile(1, t)

        @pl.when(k == 1)
        def _():
            down_load(0).wait()

        for n in range(2):
            with jax.named_scope('down'):
                down_tile(1, i, n)
                for m in (2 * n, 2 * n + 1):
                    for s in range(2):
                        back_send(i, s, m).start()
            if n == 0:
                with jax.named_scope('wait_direct'):
                    @pl.when(k == 1)
                    def _():
                        down_load(1).wait()

                    @pl.when(k < 3)
                    def _():
                        after = 4 - k
                        meta_arrived(source(after, c))
                        relay_meta(after).start()
                        for p in range(2):
                            arrived(source(after, c), p)
                            relay(after, p).start()
        return carry

    lax.fori_loop(1, 4, chunk, 0)
    with jax.named_scope('own_down'):
        own_down(0)
        own_down(1)

    cols8 = post[...]
    low = lane < CAP
    parts = []
    for k in range(EXP // 2):
        at = jnp.where(low, cols8[:, 2 * k:2 * k + 1], cols8[:, 2 * k + 1:2 * k + 2])
        here = at == (lane - jnp.where(low, 0, CAP)).astype(jnp.float32)
        parts.append((here, (2 * k + jnp.where(low, 0, 1)).astype(jnp.float32)))
    choice = [cols8[:, EXP + j:EXP + j + 1] for j in range(2)]
    picks = jnp.concatenate([jnp.concatenate([jnp.where(here & (expert == idj), 1.0, 0.0).astype(jnp.bfloat16) for here, expert in parts], axis=1) for idj in choice], axis=0)
    g0 = cols8[:, EXP + 2:EXP + 3]
    g1 = cols8[:, EXP + 3:EXP + 4]

    for m in range(NM):
        cols = msg_cols(m)
        with jax.named_scope('wait_back'):
            for other in others:
                remote(back.at[other, :, cols], back.at[other, :, cols], sb.at[0], rb.at[other, m], partner).wait_recv()
        with jax.named_scope('combine'):
            rows = back[:, :, cols].reshape(EXP * CAP, MSG[m][1])
            got = jnp.dot(picks, rows, preferred_element_type=jnp.float32)
            y_ref[:, cols] = (g0 * got[:TOK] + g1 * got[TOK:]).astype(jnp.bfloat16)

    for p in range(2):
        for k in range(3):
            own(k, p).wait_send()
        forward(p).wait_send()
        for i in range(1, 4):
            relay(i, p).wait_send()
    forward_meta().wait_send()
    for i in range(1, 4):
        relay_meta(i).wait_send()
    for own_meta in own_metas:
        own_meta.wait_send()
    for m in range(NM):
        back_partner(m).wait_send()
        for i in range(1, 4):
            for s in range(2):
                back_send(i, s, m).wait_send()


def solution(mesh):
    token_spec = P(('dp', 'ep'), None)
    expert_spec = P('ep', None, None)
    vmem = pl.BlockSpec(memory_space=pltpu.VMEM)
    anyspace = pl.BlockSpec(memory_space=pl.ANY)
    bf16, f32 = jnp.bfloat16, jnp.float32

    def local_layer(x_loc, ids_loc, gates_loc, w_up, w_down):
        return pl.pallas_call(
            moe_kernel,
            out_shape=jax.ShapeDtypeStruct((TOK, D), bf16),
            in_specs=[anyspace] * 5,
            out_specs=vmem,
            scratch_shapes=[
                pltpu.VMEM((2, TOK), jnp.int32),
                pltpu.VMEM((2, TOK), f32),
                pltpu.VMEM((D, F), bf16),
                pltpu.VMEM((F, D), bf16),
                pltpu.VMEM((EXP, TOK, D), bf16),
                pltpu.VMEM((EXP, CAP, D), bf16),
                pltpu.VMEM((2, TOK, F), bf16),
                pltpu.VMEM((TOK, D), bf16),
                pltpu.VMEM((EXP, EXP, TOK), f32),
                pltpu.VMEM((TOK, TOK), f32),
                pltpu.SemaphoreType.DMA((7, 2)),
                pltpu.SemaphoreType.DMA((EXP, 2)),
                pltpu.SemaphoreType.DMA((7,)),
                pltpu.SemaphoreType.DMA((EXP,)),
                pltpu.SemaphoreType.DMA((8 * NM,)),
                pltpu.SemaphoreType.DMA((EXP, NM)),
                pltpu.SemaphoreType.DMA((NT + 2,)),
                pltpu.SemaphoreType.DMA((3,)),
            ],
            compiler_params=pltpu.CompilerParams(vmem_limit_bytes=VMEM_LIMIT, collective_id=0, has_side_effects=True),
        )(x_loc, ids_loc.T, gates_loc.T, w_up, w_down)

    return jax.shard_map(local_layer, mesh=mesh, in_specs=(token_spec, token_spec, token_spec, expert_spec, expert_spec), out_specs=token_spec, check_vma=False)
```

```python
import functools

import jax
import jax.numpy as jnp
from jax import lax
from jax.experimental import pallas as pl
from jax.experimental.pallas import tpu as pltpu
from jax.sharding import PartitionSpec as P

MESH = pl.DeviceIdType.MESH
TOK = 128
CAP = 64
EXP = 8
D = 2304
F = 5760
NU = 1024
NT = -(-F // NU)
F_TILE = 3
AHEAD = 2
DOWN = ((0, 512), (512, 1792))
MSG = ((0, 512), (512, 640), (1152, 640), (1792, 512))
BLOCK_MSGS = ((0,), (1, 2, 3))
NM = len(MSG)
HALF = TOK // 2
VMEM_LIMIT = 66400000


def remote(src, dst, send_sem, recv_sem, dev):
    return pltpu.make_async_remote_copy(src_ref=src, dst_ref=dst, send_sem=send_sem, recv_sem=recv_sem, device_id={'ep': dev}, device_id_type=MESH)


def moe_kernel(x_hbm, ids_hbm, gates_hbm, wu_hbm, wd_hbm, y_ref, ids_ref, gates_ref, wu, wd, xg, back, hid, xs, posg, post, sx, rx, sm, rm, sb, rb, sw, sl):
    me = lax.axis_index('ep')
    c = lax.rem(me, 2)
    x = lax.rem(me // 2, 2)
    y = me // 4

    def dev(yy, xx, cc):
        return yy * 4 + xx * 2 + cc

    partner = dev(y, x, 1 - c)
    first = dev(lax.rem(y + c, 2), lax.rem(x + 1 - c, 2), c)
    second = dev(lax.rem(y + 1 - c, 2), lax.rem(x + c, 2), c)
    others = [dev(lax.rem(y + dy, 2), lax.rem(x + dx, 2), lax.rem(c + dc, 2)) for dy, dx, dc in ((0, 0, 1), (0, 1, 0), (1, 0, 0), (0, 1, 1), (1, 0, 1), (1, 1, 0), (1, 1, 1))]

    def source(i, cc):
        lo, hi = lax.rem(i, 2), i // 2
        fx = lo * (1 - cc) + hi * cc
        fy = hi * (1 - cc) + lo * cc
        return dev(lax.rem(y + fy, 2), lax.rem(x + fx, 2), cc)

    barrier = pltpu.get_barrier_semaphore()
    for other in (partner, first, second):
        pl.semaphore_signal(barrier, inc=1, device_id={'ep': other}, device_id_type=MESH)
    ids_load = pltpu.make_async_copy(ids_hbm, ids_ref, sl.at[1])
    gates_load = pltpu.make_async_copy(gates_hbm, gates_ref, sl.at[2])
    ids_load.start()
    gates_load.start()
    own_load = pltpu.make_async_copy(x_hbm, xg.at[me], sl.at[0])
    own_load.start()

    def up_cols(t):
        return pl.ds(t * NU, min(NU, F - t * NU))

    def down_cols(n):
        return pl.ds(*DOWN[n])

    def msg_cols(m):
        return pl.ds(*MSG[m])

    def up_load(t):
        return pltpu.make_async_copy(wu_hbm.at[0, :, up_cols(t)], wu.at[:, up_cols(t)], sw.at[t])

    def down_load(n):
        return pltpu.make_async_copy(wd_hbm.at[0, :, down_cols(n)], wd.at[:, down_cols(n)], sw.at[NT + n])

    with jax.named_scope('own_load'):
        own_load.wait()
    for t in range(AHEAD):
        up_load(t).start()
    with jax.named_scope('barrier'):
        pl.semaphore_wait(barrier, 3)

    def block(s, k, p, to):
        rows = pl.ds(p * HALF, HALF)
        return remote(xg.at[s, rows], xg.at[s, rows], sx.at[k, p], rx.at[s, p], to)

    def own(k, p):
        return block(me, k, p, (first, partner, second)[k])

    def forward(p):
        return block(source(1, c), 3, p, second)

    def relay(i, p):
        return block(source(i, c), 3 + i, p, partner)

    def arrived(s, p):
        block(s, 0, p, partner).wait_recv()

    def meta_arrived(s):
        meta(s, 0, partner).wait_recv()

    def meta(s, k, to):
        return remote(posg.at[s], posg.at[s], sm.at[k], rm.at[s], to)

    own_metas = [meta(me, k, to) for k, to in enumerate((first, partner, second))]

    def forward_meta():
        return meta(source(1, c), 3, second)

    def relay_meta(i):
        return meta(source(i, c), 3 + i, partner)

    def back_send(i, s, m):
        return remote(xg.at[source(i, 1 - c), pl.ds(s * CAP, CAP), msg_cols(m)], back.at[me, :, msg_cols(m)], sb.at[(i * 2 + s) * NM + m], rb.at[me, m], source(i, s))

    def back_partner(m):
        return remote(xg.at[partner, pl.ds(pl.multiple_of((1 - c) * CAP, CAP), CAP), msg_cols(m)], back.at[me, :, msg_cols(m)], sb.at[m], rb.at[me, m], partner)

    def gather(i):
        for s in range(2):
            s_id = source(i, s)
            where = posg[s_id, pl.ds(me, 1), :]
            rank_row = lax.broadcasted_iota(jnp.int32, (CAP, TOK), 0).astype(jnp.float32)
            pick = jnp.where(rank_row == where, 1.0, 0.0).astype(jnp.bfloat16)
            xs[s * CAP:(s + 1) * CAP, :] = jnp.dot(pick, xg[s_id], preferred_element_type=jnp.float32).astype(jnp.bfloat16)

    def up_tile(h, t):
        z = jnp.dot(xs[...], wu[:, up_cols(t)], preferred_element_type=jnp.float32)
        hid[h, :, up_cols(t)] = jax.nn.gelu(z, approximate=True).astype(jnp.bfloat16)

    def down_tile(h, i, n):
        xg[source(i, 1 - c), :, down_cols(n)] = jnp.dot(hid[h], wd[:, down_cols(n)], preferred_element_type=jnp.float32).astype(jnp.bfloat16)

    def own_down(n):
        down_tile(0, 0, n)
        for m in BLOCK_MSGS[n]:
            back_partner(m).start()
        back[me, :, down_cols(n)] = xg[partner, pl.ds(pl.multiple_of(c * CAP, CAP), CAP), down_cols(n)]

    own(0, 0).start()
    own(1, 0).start()
    for t in range(AHEAD, 4):
        up_load(t).start()
    ids_load.wait()
    gates_load.wait()
    lane = lax.broadcasted_iota(jnp.int32, (TOK, TOK), 1)
    row = lax.broadcasted_iota(jnp.int32, (TOK, TOK), 0)
    expert_row = lax.broadcasted_iota(jnp.int32, (EXP, TOK), 0)
    hit = (ids_ref[0:1, :] == expert_row) | (ids_ref[1:2, :] == expert_row)
    upper = jnp.where(row < lane, 1.0, 0.0).astype(jnp.bfloat16)
    rank = jnp.dot(jnp.where(hit, 1.0, 0.0).astype(jnp.bfloat16), upper, preferred_element_type=jnp.float32)
    slots = jnp.where(hit, rank, -1.0)
    posg[me] = slots
    pad = jnp.zeros((TOK - EXP - 4, TOK), jnp.float32)
    post[...] = jnp.concatenate([slots, ids_ref[...].astype(jnp.float32), gates_ref[...], pad], axis=0).T
    for own_meta in own_metas:
        own_meta.start()
    own(0, 1).start()
    own(1, 1).start()
    with jax.named_scope('wait_partner'):
        meta_arrived(partner)
        for p in range(2):
            arrived(partner, p)
    with jax.named_scope('up0'):
        gather(0)
        for t in range(NT):
            up_load(t).wait()
            if t < 2:
                up_load(4 + t).start()
            if t == 2:
                down_load(0).start()
            if t == F_TILE:
                with jax.named_scope('wait_f0'):
                    meta_arrived(source(1, c))
                    arrived(source(1, c), 0)
                forward_meta().start()
                forward(0).start()
                relay_meta(1).start()
                relay(1, 0).start()
            if t == NT - 1:
                down_load(1).start()
                with jax.named_scope('wait_f1'):
                    arrived(source(1, c), 1)
                    forward(1).start()
                    relay(1, 1).start()
                    for p in range(2):
                        own(2, p).start()
            up_tile(0, t)
    def chunk(k, carry):
        i = jnp.where(k == 1, 1, 5 - k)
        with jax.named_scope('wait_chunk'):
            meta_arrived(source(i, 1 - c))
            for p in range(2):
                arrived(source(i, 1 - c), p)
        with jax.named_scope('up'):
            gather(i)
            for t in range(NT):
                up_tile(1, t)

        @pl.when(k == 1)
        def _():
            down_load(0).wait()

        for n in range(2):
            with jax.named_scope('down'):
                down_tile(1, i, n)

                @pl.when(k < 3)
                def _():
                    for m in BLOCK_MSGS[n]:
                        for s in range(2):
                            back_send(i, s, m).start()
            if n == 0:
                with jax.named_scope('wait_direct'):
                    @pl.when(k == 1)
                    def _():
                        down_load(1).wait()

                    @pl.when(k < 3)
                    def _():
                        after = 4 - k
                        meta_arrived(source(after, c))
                        relay_meta(after).start()
                        for p in range(2):
                            arrived(source(after, c), p)
                            relay(after, p).start()
        @pl.when(k == 3)
        def _():
            for m in range(NM):
                for s in range(2):
                    back_send(i, s, m).start()

        return carry

    lax.fori_loop(1, 4, chunk, 0)
    with jax.named_scope('own_down'):
        own_down(0)
        own_down(1)

    cols8 = post[...]
    low = lane < CAP
    parts = []
    for k in range(EXP // 2):
        at = jnp.where(low, cols8[:, 2 * k:2 * k + 1], cols8[:, 2 * k + 1:2 * k + 2])
        here = at == (lane - jnp.where(low, 0, CAP)).astype(jnp.float32)
        parts.append((here, (2 * k + jnp.where(low, 0, 1)).astype(jnp.float32)))
    choice = [cols8[:, EXP + j:EXP + j + 1] for j in range(2)]
    picks = jnp.concatenate([jnp.concatenate([jnp.where(here & (expert == idj), 1.0, 0.0).astype(jnp.bfloat16) for here, expert in parts], axis=1) for idj in choice], axis=0)
    g0 = cols8[:, EXP + 2:EXP + 3]
    g1 = cols8[:, EXP + 3:EXP + 4]

    for m in range(NM):
        cols = msg_cols(m)
        with jax.named_scope('wait_back'):
            for other in others:
                remote(back.at[other, :, cols], back.at[other, :, cols], sb.at[0], rb.at[other, m], partner).wait_recv()
        with jax.named_scope('combine'):
            rows = back[:, :, cols].reshape(EXP * CAP, MSG[m][1])
            got = jnp.dot(picks, rows, preferred_element_type=jnp.float32)
            y_ref[:, cols] = (g0 * got[:TOK] + g1 * got[TOK:]).astype(jnp.bfloat16)

    for p in range(2):
        for k in range(3):
            own(k, p).wait_send()
        forward(p).wait_send()
        for i in range(1, 4):
            relay(i, p).wait_send()
    forward_meta().wait_send()
    for i in range(1, 4):
        relay_meta(i).wait_send()
    for own_meta in own_metas:
        own_meta.wait_send()
    for m in range(NM):
        back_partner(m).wait_send()
        for i in range(1, 4):
            for s in range(2):
                back_send(i, s, m).wait_send()


def solution(mesh):
    token_spec = P(('dp', 'ep'), None)
    expert_spec = P('ep', None, None)
    vmem = pl.BlockSpec(memory_space=pltpu.VMEM)
    anyspace = pl.BlockSpec(memory_space=pl.ANY)
    bf16, f32 = jnp.bfloat16, jnp.float32

    def local_layer(x_loc, ids_loc, gates_loc, w_up, w_down):
        return pl.pallas_call(
            moe_kernel,
            out_shape=pltpu.VMEM((TOK, D), bf16),
            in_specs=[anyspace] * 5,
            out_specs=vmem,
            scratch_shapes=[
                pltpu.VMEM((2, TOK), jnp.int32),
                pltpu.VMEM((2, TOK), f32),
                pltpu.VMEM((D, F), bf16),
                pltpu.VMEM((F, D), bf16),
                pltpu.VMEM((EXP, TOK, D), bf16),
                pltpu.VMEM((EXP, CAP, D), bf16),
                pltpu.VMEM((2, TOK, F), bf16),
                pltpu.VMEM((TOK, D), bf16),
                pltpu.VMEM((EXP, EXP, TOK), f32),
                pltpu.VMEM((TOK, TOK), f32),
                pltpu.SemaphoreType.DMA((7, 2)),
                pltpu.SemaphoreType.DMA((EXP, 2)),
                pltpu.SemaphoreType.DMA((7,)),
                pltpu.SemaphoreType.DMA((EXP,)),
                pltpu.SemaphoreType.DMA((8 * NM,)),
                pltpu.SemaphoreType.DMA((EXP, NM)),
                pltpu.SemaphoreType.DMA((NT + 2,)),
                pltpu.SemaphoreType.DMA((3,)),
            ],
            compiler_params=pltpu.CompilerParams(vmem_limit_bytes=VMEM_LIMIT, collective_id=0, has_side_effects=True),
        )(x_loc, ids_loc.T, gates_loc.T, w_up, w_down)

    return jax.shard_map(local_layer, mesh=mesh, in_specs=(token_spec, token_spec, token_spec, expert_spec, expert_spec), out_specs=token_spec, check_vma=False)
```

```python
import functools

import jax
import jax.numpy as jnp
from jax import lax
from jax.experimental import pallas as pl
from jax.experimental.pallas import tpu as pltpu
from jax.sharding import PartitionSpec as P

MESH = pl.DeviceIdType.MESH
TOK = 128
CAP = 64
EXP = 8
D = 2304
F = 5760
NU = 1024
NT = -(-F // NU)
F_TILE = 3
AHEAD = 2
DOWN = ((0, 512), (512, 512), (1024, 1280))
MSG = ((0, 512), (512, 512), (1024, 640), (1664, 384), (2048, 256))
BLOCK_MSGS = ((0,), (1,), (2, 3, 4))
NM = len(MSG)
HALF = TOK // 2
VMEM_LIMIT = 66400000


def remote(src, dst, send_sem, recv_sem, dev):
    return pltpu.make_async_remote_copy(src_ref=src, dst_ref=dst, send_sem=send_sem, recv_sem=recv_sem, device_id={'ep': dev}, device_id_type=MESH)


def moe_kernel(x_hbm, ids_hbm, gates_hbm, wu_hbm, wd_hbm, y_ref, ids_ref, gates_ref, wu, wd, xg, back, hid, xs, posg, post, send_x, send_m, send_b, rf, rx, rm, rb, sw, sl):
    me = lax.axis_index('ep')
    c = lax.rem(me, 2)
    x = lax.rem(me // 2, 2)
    y = me // 4

    def dev(yy, xx, cc):
        return yy * 4 + xx * 2 + cc

    partner = dev(y, x, 1 - c)
    first = dev(lax.rem(y + c, 2), lax.rem(x + 1 - c, 2), c)
    second = dev(lax.rem(y + 1 - c, 2), lax.rem(x + c, 2), c)
    def source(i, cc):
        lo, hi = lax.rem(i, 2), i // 2
        fx = lo * (1 - cc) + hi * cc
        fy = hi * (1 - cc) + lo * cc
        return dev(lax.rem(y + fy, 2), lax.rem(x + fx, 2), cc)

    barrier = pltpu.get_barrier_semaphore()
    for other in (partner, first, second):
        pl.semaphore_signal(barrier, inc=1, device_id={'ep': other}, device_id_type=MESH)
    ids_load = pltpu.make_async_copy(ids_hbm, ids_ref, sl.at[1])
    gates_load = pltpu.make_async_copy(gates_hbm, gates_ref, sl.at[2])
    ids_load.start()
    gates_load.start()
    own_load = pltpu.make_async_copy(x_hbm, xg.at[me], sl.at[0])
    own_load.start()

    def up_cols(t):
        return pl.ds(t * NU, min(NU, F - t * NU))

    def down_cols(n):
        return pl.ds(*DOWN[n])

    def msg_cols(m):
        return pl.ds(*MSG[m])

    def up_load(t):
        return pltpu.make_async_copy(wu_hbm.at[0, :, up_cols(t)], wu.at[:, up_cols(t)], sw.at[t])

    def down_load(n):
        cols = pl.ds(*((0, 1024), (1024, 1280))[n])
        return pltpu.make_async_copy(wd_hbm.at[0, :, cols], wd.at[:, cols], sw.at[NT + n])

    with jax.named_scope('own_load'):
        own_load.wait()
    for t in range(AHEAD):
        up_load(t).start()
    with jax.named_scope('barrier'):
        pl.semaphore_wait(barrier, 3)

    def half(s, p, recv_sem, to):
        rows = pl.ds(p * HALF, HALF)
        return remote(xg.at[s, rows], xg.at[s, rows], send_x, recv_sem, to)

    def block(s, to):
        return remote(xg.at[s], xg.at[s], send_x, rx.at[s], to)

    def arrived(s):
        block(s, partner).wait_recv()

    def meta_arrived(s):
        meta(s, partner).wait_recv()

    def meta(s, to):
        return remote(posg.at[s], posg.at[s], send_m, rm.at[s], to)

    def back_send(i, s, m):
        return remote(xg.at[source(i, 1 - c), pl.ds(s * CAP, CAP), msg_cols(m)], back.at[me, :, msg_cols(m)], send_b, rb.at[m], source(i, s))

    def back_partner(m):
        return remote(xg.at[partner, pl.ds(pl.multiple_of((1 - c) * CAP, CAP), CAP), msg_cols(m)], back.at[me, :, msg_cols(m)], send_b, rb.at[m], partner)

    def gather(i, s):
        s_id = source(i, s)
        where = posg[s_id, pl.ds(me, 1), :]
        rank_row = lax.broadcasted_iota(jnp.int32, (CAP, TOK), 0).astype(jnp.float32)
        pick = jnp.where(rank_row == where, 1.0, 0.0).astype(jnp.bfloat16)
        xs[s * CAP:(s + 1) * CAP, :] = jnp.dot(pick, xg[s_id], preferred_element_type=jnp.float32).astype(jnp.bfloat16)

    def up_tile(h, t):
        z = jnp.dot(xs[...], wu[:, up_cols(t)], preferred_element_type=jnp.float32)
        hid[h, :, up_cols(t)] = jax.nn.gelu(z, approximate=True).astype(jnp.bfloat16)

    def down_tile(h, i, n):
        xg[source(i, 1 - c), :, down_cols(n)] = jnp.dot(hid[h], wd[:, down_cols(n)], preferred_element_type=jnp.float32).astype(jnp.bfloat16)

    def own_down(n):
        down_tile(0, 0, n)
        for m in BLOCK_MSGS[n]:
            back_partner(m).start()
        back[me, :, down_cols(n)] = xg[partner, pl.ds(pl.multiple_of(c * CAP, CAP), CAP), down_cols(n)]

    half(me, 0, rf, first).start()
    block(me, partner).start()
    for t in range(AHEAD, 4):
        up_load(t).start()
    ids_load.wait()
    gates_load.wait()
    lane = lax.broadcasted_iota(jnp.int32, (TOK, TOK), 1)
    row = lax.broadcasted_iota(jnp.int32, (TOK, TOK), 0)
    expert_row = lax.broadcasted_iota(jnp.int32, (EXP, TOK), 0)
    hit = (ids_ref[0:1, :] == expert_row) | (ids_ref[1:2, :] == expert_row)
    upper = jnp.where(row < lane, 1.0, 0.0).astype(jnp.bfloat16)
    rank = jnp.dot(jnp.where(hit, 1.0, 0.0).astype(jnp.bfloat16), upper, preferred_element_type=jnp.float32)
    slots = jnp.where(hit, rank, -1.0)
    posg[me] = slots
    pad = jnp.zeros((TOK - EXP - 4, TOK), jnp.float32)
    post[...] = jnp.concatenate([slots, ids_ref[...].astype(jnp.float32), gates_ref[...], pad], axis=0).T
    for to in (first, partner, second):
        meta(me, to).start()
    half(me, 1, rx.at[me], first).start()
    near = source(1, c)
    with jax.named_scope('wait_partner'):
        meta_arrived(partner)
        arrived(partner)
    with jax.named_scope('up0'):
        gather(0, 0)
        gather(0, 1)
        for t in range(NT):
            up_load(t).wait()
            if t < 2:
                up_load(4 + t).start()
            if t == 2:
                down_load(0).start()
            if t == F_TILE:
                with jax.named_scope('wait_f0'):
                    meta_arrived(near)
                    half(near, 0, rf, partner).wait_recv()
                for to in (second, partner):
                    meta(near, to).start()
                    half(near, 0, rx.at[near], to).start()
            if t == NT - 1:
                down_load(1).start()
                with jax.named_scope('wait_f1'):
                    half(near, 1, rx.at[near], partner).wait_recv()
                    for to in (second, partner):
                        half(near, 1, rx.at[near], to).start()
                    block(me, second).start()
            up_tile(0, t)

    def chunk(k, carry):
        i = jnp.where(k == 1, 1, 5 - k)
        with jax.named_scope('wait_chunk'):
            meta_arrived(source(i, 1 - c))
            arrived(source(i, 1 - c))
        with jax.named_scope('up'):
            gather(i, 0)
            gather(i, 1)
            for t in range(NT):
                up_tile(1, t)

        @pl.when(k == 1)
        def _():
            down_load(0).wait()

        for n in range(len(DOWN)):
            with jax.named_scope('down'):
                down_tile(1, i, n)

                @pl.when(k < 3)
                def _():
                    for m in BLOCK_MSGS[n]:
                        for s in range(2):
                            back_send(i, s, m).start()
            if n == 0:
                with jax.named_scope('wait_direct'):
                    @pl.when(k == 1)
                    def _():
                        down_load(1).wait()

                    @pl.when(k < 3)
                    def _():
                        after = source(4 - k, c)
                        meta_arrived(after)
                        arrived(after)
                        meta(after, partner).start()
                        block(after, partner).start()
        @pl.when(k == 3)
        def _():
            for m in range(NM):
                for s in range(2):
                    back_send(i, s, m).start()

        return carry

    lax.fori_loop(1, 4, chunk, 0)
    with jax.named_scope('own_down'):
        for n in range(len(DOWN)):
            own_down(n)

    cols8 = post[...]
    low = lane < CAP
    parts = []
    for k in range(EXP // 2):
        at = jnp.where(low, cols8[:, 2 * k:2 * k + 1], cols8[:, 2 * k + 1:2 * k + 2])
        here = at == (lane - jnp.where(low, 0, CAP)).astype(jnp.float32)
        parts.append((here, (2 * k + jnp.where(low, 0, 1)).astype(jnp.float32)))
    choice = [cols8[:, EXP + j:EXP + j + 1] for j in range(2)]
    picks = jnp.concatenate([jnp.concatenate([jnp.where(here & (expert == idj), 1.0, 0.0).astype(jnp.bfloat16) for here, expert in parts], axis=1) for idj in choice], axis=0)
    g0 = cols8[:, EXP + 2:EXP + 3]
    g1 = cols8[:, EXP + 3:EXP + 4]

    for m in range(NM):
        cols = msg_cols(m)
        with jax.named_scope('wait_back'):
            seven = back.at[pl.ds(0, EXP - 1), :, cols]
            remote(seven, seven, send_b, rb.at[m], partner).wait_recv()
        with jax.named_scope('combine'):
            rows = back[:, :, cols].reshape(EXP * CAP, MSG[m][1])
            got = jnp.dot(picks, rows, preferred_element_type=jnp.float32)
            y_ref[:, cols] = (g0 * got[:TOK] + g1 * got[TOK:]).astype(jnp.bfloat16)

    for sent, sem in ((xg, send_x), (posg, send_m), (back, send_b)):
        seven = sent.at[pl.ds(0, EXP - 1)]
        remote(seven, seven, sem, rf, partner).wait_send()


def solution(mesh):
    token_spec = P(('dp', 'ep'), None)
    expert_spec = P('ep', None, None)
    vmem = pl.BlockSpec(memory_space=pltpu.VMEM)
    anyspace = pl.BlockSpec(memory_space=pl.ANY)
    bf16, f32 = jnp.bfloat16, jnp.float32

    def local_layer(x_loc, ids_loc, gates_loc, w_up, w_down):
        return pl.pallas_call(
            moe_kernel,
            out_shape=pltpu.VMEM((TOK, D), bf16),
            in_specs=[anyspace] * 5,
            out_specs=vmem,
            scratch_shapes=[
                pltpu.VMEM((2, TOK), jnp.int32),
                pltpu.VMEM((2, TOK), f32),
                pltpu.VMEM((D, F), bf16),
                pltpu.VMEM((F, D), bf16),
                pltpu.VMEM((EXP, TOK, D), bf16),
                pltpu.VMEM((EXP, CAP, D), bf16),
                pltpu.VMEM((2, TOK, F), bf16),
                pltpu.VMEM((TOK, D), bf16),
                pltpu.VMEM((EXP, EXP, TOK), f32),
                pltpu.VMEM((TOK, TOK), f32),
                pltpu.SemaphoreType.DMA,
                pltpu.SemaphoreType.DMA,
                pltpu.SemaphoreType.DMA,
                pltpu.SemaphoreType.DMA,
                pltpu.SemaphoreType.DMA((EXP,)),
                pltpu.SemaphoreType.DMA((EXP,)),
                pltpu.SemaphoreType.DMA((NM,)),
                pltpu.SemaphoreType.DMA((NT + 2,)),
                pltpu.SemaphoreType.DMA((3,)),
            ],
            compiler_params=pltpu.CompilerParams(vmem_limit_bytes=VMEM_LIMIT, collective_id=0, has_side_effects=True),
        )(x_loc, ids_loc.T, gates_loc.T, w_up, w_down)

    return jax.shard_map(local_layer, mesh=mesh, in_specs=(token_spec, token_spec, token_spec, expert_spec, expert_spec), out_specs=token_spec, check_vma=False)
```

```python
import functools

import jax
import jax.numpy as jnp
from jax import lax
from jax.experimental import pallas as pl
from jax.experimental.pallas import tpu as pltpu
from jax.sharding import PartitionSpec as P

MESH = pl.DeviceIdType.MESH
TOK = 128
CAP = 64
EXP = 8
D = 2304
F = 5760
NU = 1024
NT = -(-F // NU)
F_TILE = 3
AHEAD = 2
DOWN = ((0, 512), (512, 512), (1024, 1280))
MSG = ((0, 512), (512, 512), (1024, 640), (1664, 384), (2048, 256))
BLOCK_MSGS = ((0,), (1,), (2, 3, 4))
NM = len(MSG)
HALF = TOK // 2
VMEM_LIMIT = 66400000


def remote(src, dst, send_sem, recv_sem, dev):
    return pltpu.make_async_remote_copy(src_ref=src, dst_ref=dst, send_sem=send_sem, recv_sem=recv_sem, device_id={'ep': dev}, device_id_type=MESH)


def moe_kernel(x_hbm, ids_hbm, gates_hbm, wu_hbm, wd_hbm, y_ref, ids_ref, gates_ref, wu, wd, xg, back, hid, xs, posg, post, send_x, send_m, send_b, rf, rx, rm, rb, sw, sl):
    me = lax.axis_index('ep')
    c = lax.rem(me, 2)
    x = lax.rem(me // 2, 2)
    y = me // 4

    def dev(yy, xx, cc):
        return yy * 4 + xx * 2 + cc

    partner = dev(y, x, 1 - c)
    first = dev(lax.rem(y + 1 - c, 2), lax.rem(x + c, 2), c)
    second = dev(lax.rem(y + c, 2), lax.rem(x + 1 - c, 2), c)
    def source(i, cc):
        lo, hi = lax.rem(i, 2), i // 2
        fy = lo * (1 - cc) + hi * cc
        fx = hi * (1 - cc) + lo * cc
        return dev(lax.rem(y + fy, 2), lax.rem(x + fx, 2), cc)

    own_load = pltpu.make_async_copy(x_hbm, xg.at[me], sl.at[0])
    own_load.start()
    barrier = pltpu.get_barrier_semaphore()
    for other in (partner, first, second):
        pl.semaphore_signal(barrier, inc=1, device_id={'ep': other}, device_id_type=MESH)
    ids_load = pltpu.make_async_copy(ids_hbm, ids_ref, sl.at[1])
    gates_load = pltpu.make_async_copy(gates_hbm, gates_ref, sl.at[2])
    ids_load.start()
    gates_load.start()
    def up_cols(t):
        return pl.ds(t * NU, min(NU, F - t * NU))

    def down_cols(n):
        return pl.ds(*DOWN[n])

    def msg_cols(m):
        return pl.ds(*MSG[m])

    def up_load(t):
        return pltpu.make_async_copy(wu_hbm.at[0, :, up_cols(t)], wu.at[:, up_cols(t)], sw.at[t])

    def down_load(n):
        cols = pl.ds(*((0, 1024), (1024, 1280))[n])
        return pltpu.make_async_copy(wd_hbm.at[0, :, cols], wd.at[:, cols], sw.at[NT + n])

    with jax.named_scope('own_load'):
        own_load.wait()
    for t in range(AHEAD):
        up_load(t).start()
    with jax.named_scope('barrier'):
        pl.semaphore_wait(barrier, 3)

    def half(s, p, recv_sem, to):
        rows = pl.ds(p * HALF, HALF)
        return remote(xg.at[s, rows], xg.at[s, rows], send_x, recv_sem, to)

    def block(s, to):
        return remote(xg.at[s], xg.at[s], send_x, rx.at[s], to)

    def arrived(s):
        block(s, partner).wait_recv()

    def meta_arrived(s):
        meta(s, partner).wait_recv()

    def meta(s, to):
        return remote(posg.at[s], posg.at[s], send_m, rm.at[s], to)

    def back_send(i, s, m):
        return remote(xg.at[source(i, 1 - c), pl.ds(s * CAP, CAP), msg_cols(m)], back.at[me, :, msg_cols(m)], send_b, rb.at[m], source(i, s))

    def back_partner(m):
        return remote(xg.at[partner, pl.ds(pl.multiple_of((1 - c) * CAP, CAP), CAP), msg_cols(m)], back.at[me, :, msg_cols(m)], send_b, rb.at[m], partner)

    def gather(i, s):
        s_id = source(i, s)
        where = posg[s_id, pl.ds(me, 1), :]
        rank_row = lax.broadcasted_iota(jnp.int32, (CAP, TOK), 0).astype(jnp.float32)
        pick = jnp.where(rank_row == where, 1.0, 0.0).astype(jnp.bfloat16)
        xs[s * CAP:(s + 1) * CAP, :] = jnp.dot(pick, xg[s_id], preferred_element_type=jnp.float32).astype(jnp.bfloat16)

    def up_tile(h, t):
        z = jnp.dot(xs[...], wu[:, up_cols(t)], preferred_element_type=jnp.float32)
        hid[h, :, up_cols(t)] = jax.nn.gelu(z, approximate=True).astype(jnp.bfloat16)

    def down_tile(h, i, n):
        xg[source(i, 1 - c), :, down_cols(n)] = jnp.dot(hid[h], wd[:, down_cols(n)], preferred_element_type=jnp.float32).astype(jnp.bfloat16)

    def own_down(n):
        down_tile(0, 0, n)
        for m in BLOCK_MSGS[n]:
            back_partner(m).start()
        back[me, :, down_cols(n)] = xg[partner, pl.ds(pl.multiple_of(c * CAP, CAP), CAP), down_cols(n)]

    half(me, 0, rf, first).start()
    block(me, partner).start()
    for t in range(AHEAD, 4):
        up_load(t).start()
    ids_load.wait()
    gates_load.wait()
    lane = lax.broadcasted_iota(jnp.int32, (TOK, TOK), 1)
    row = lax.broadcasted_iota(jnp.int32, (TOK, TOK), 0)
    expert_row = lax.broadcasted_iota(jnp.int32, (EXP, TOK), 0)
    hit = (ids_ref[0:1, :] == expert_row) | (ids_ref[1:2, :] == expert_row)
    upper = jnp.where(row < lane, 1.0, 0.0).astype(jnp.bfloat16)
    rank = jnp.dot(jnp.where(hit, 1.0, 0.0).astype(jnp.bfloat16), upper, preferred_element_type=jnp.float32)
    slots = jnp.where(hit, rank, -1.0)
    posg[me] = slots
    pad = jnp.zeros((TOK - EXP - 4, TOK), jnp.float32)
    post[...] = jnp.concatenate([slots, ids_ref[...].astype(jnp.float32), gates_ref[...], pad], axis=0).T
    for to in (first, partner, second):
        meta(me, to).start()
    half(me, 1, rx.at[me], first).start()
    near = source(1, c)
    with jax.named_scope('wait_partner'):
        meta_arrived(partner)
        arrived(partner)
    with jax.named_scope('up0'):
        gather(0, 0)
        gather(0, 1)
        for t in range(NT):
            up_load(t).wait()
            if t < 2:
                up_load(4 + t).start()
            if t == 2:
                down_load(0).start()
            if t == F_TILE:
                with jax.named_scope('wait_f0'):
                    meta_arrived(near)
                    half(near, 0, rf, partner).wait_recv()
                for to in (second, partner):
                    meta(near, to).start()
                    half(near, 0, rx.at[near], to).start()
            if t == NT - 1:
                down_load(1).start()
                with jax.named_scope('wait_f1'):
                    half(near, 1, rx.at[near], partner).wait_recv()
                    for to in (second, partner):
                        half(near, 1, rx.at[near], to).start()
                    block(me, second).start()
            up_tile(0, t)

    def chunk(k, carry):
        i = jnp.where(k == 1, 1, 5 - k)
        with jax.named_scope('wait_chunk'):
            meta_arrived(source(i, 1 - c))
            arrived(source(i, 1 - c))
        with jax.named_scope('up'):
            gather(i, 0)
            gather(i, 1)
            for t in range(NT):
                up_tile(1, t)

        @pl.when(k == 1)
        def _():
            down_load(0).wait()

        for n in range(len(DOWN)):
            with jax.named_scope('down'):
                down_tile(1, i, n)

                @pl.when(k < 3)
                def _():
                    for m in BLOCK_MSGS[n]:
                        for s in range(2):
                            back_send(i, s, m).start()
            if n == 0:
                with jax.named_scope('wait_direct'):
                    @pl.when(k == 1)
                    def _():
                        down_load(1).wait()

                    @pl.when(k < 3)
                    def _():
                        after = source(4 - k, c)
                        meta_arrived(after)
                        arrived(after)
                        meta(after, partner).start()
                        block(after, partner).start()
        @pl.when(k == 3)
        def _():
            for m in range(NM):
                for s in range(2):
                    back_send(i, s, m).start()

        return carry

    lax.fori_loop(1, 4, chunk, 0)
    with jax.named_scope('own_down'):
        for n in range(len(DOWN)):
            own_down(n)

    cols8 = post[...]
    low = lane < CAP
    parts = []
    for k in range(EXP // 2):
        at = jnp.where(low, cols8[:, 2 * k:2 * k + 1], cols8[:, 2 * k + 1:2 * k + 2])
        here = at == (lane - jnp.where(low, 0, CAP)).astype(jnp.float32)
        parts.append((here, (2 * k + jnp.where(low, 0, 1)).astype(jnp.float32)))
    choice = [cols8[:, EXP + j:EXP + j + 1] for j in range(2)]
    picks = jnp.concatenate([jnp.concatenate([jnp.where(here & (expert == idj), 1.0, 0.0).astype(jnp.bfloat16) for here, expert in parts], axis=1) for idj in choice], axis=0)
    g0 = cols8[:, EXP + 2:EXP + 3]
    g1 = cols8[:, EXP + 3:EXP + 4]

    for m in range(NM):
        cols = msg_cols(m)
        with jax.named_scope('wait_back'):
            seven = back.at[pl.ds(0, EXP - 1), :, cols]
            remote(seven, seven, send_b, rb.at[m], partner).wait_recv()
        with jax.named_scope('combine'):
            rows = back[:, :, cols].reshape(EXP * CAP, MSG[m][1])
            got = jnp.dot(picks, rows, preferred_element_type=jnp.float32)
            y_ref[:, cols] = (g0 * got[:TOK] + g1 * got[TOK:]).astype(jnp.bfloat16)

    for sent, sem in ((xg, send_x), (posg, send_m), (back, send_b)):
        seven = sent.at[pl.ds(0, EXP - 1)]
        remote(seven, seven, sem, rf, partner).wait_send()


def solution(mesh):
    token_spec = P(('dp', 'ep'), None)
    expert_spec = P('ep', None, None)
    vmem = pl.BlockSpec(memory_space=pltpu.VMEM)
    anyspace = pl.BlockSpec(memory_space=pl.ANY)
    bf16, f32 = jnp.bfloat16, jnp.float32

    def local_layer(x_loc, ids_loc, gates_loc, w_up, w_down):
        return pl.pallas_call(
            moe_kernel,
            out_shape=pltpu.VMEM((TOK, D), bf16),
            in_specs=[anyspace] * 5,
            out_specs=vmem,
            scratch_shapes=[
                pltpu.VMEM((2, TOK), jnp.int32),
                pltpu.VMEM((2, TOK), f32),
                pltpu.VMEM((D, F), bf16),
                pltpu.VMEM((F, D), bf16),
                pltpu.VMEM((EXP, TOK, D), bf16),
                pltpu.VMEM((EXP, CAP, D), bf16),
                pltpu.VMEM((2, TOK, F), bf16),
                pltpu.VMEM((TOK, D), bf16),
                pltpu.VMEM((EXP, EXP, TOK), f32),
                pltpu.VMEM((TOK, TOK), f32),
                pltpu.SemaphoreType.DMA,
                pltpu.SemaphoreType.DMA,
                pltpu.SemaphoreType.DMA,
                pltpu.SemaphoreType.DMA,
                pltpu.SemaphoreType.DMA((EXP,)),
                pltpu.SemaphoreType.DMA((EXP,)),
                pltpu.SemaphoreType.DMA((NM,)),
                pltpu.SemaphoreType.DMA((NT + 2,)),
                pltpu.SemaphoreType.DMA((3,)),
            ],
            compiler_params=pltpu.CompilerParams(vmem_limit_bytes=VMEM_LIMIT, collective_id=0, has_side_effects=True),
        )(x_loc, ids_loc.T, gates_loc.T, w_up, w_down)

    return jax.shard_map(local_layer, mesh=mesh, in_specs=(token_spec, token_spec, token_spec, expert_spec, expert_spec), out_specs=token_spec, check_vma=False)
```

```python
import functools

import jax
import jax.numpy as jnp
from jax import lax
from jax.experimental import pallas as pl
from jax.experimental.pallas import tpu as pltpu
from jax.sharding import PartitionSpec as P

MESH = pl.DeviceIdType.MESH
TOK = 128
CAP = 64
EXP = 8
D = 2304
F = 5760
NU = 1024
NT = -(-F // NU)
F_TILE = 3
AHEAD = 2
DOWN = ((0, 512), (512, 512), (1024, 1280))
MSG = ((0, 512), (512, 512), (1024, 640), (1664, 384), (2048, 256))
BLOCK_MSGS = ((0,), (1,), (2, 3, 4))
NM = len(MSG)
HALF = TOK // 2
VMEM_LIMIT = 66400000


def remote(src, dst, send_sem, recv_sem, dev):
    return pltpu.make_async_remote_copy(src_ref=src, dst_ref=dst, send_sem=send_sem, recv_sem=recv_sem, device_id={'ep': dev}, device_id_type=MESH)


def moe_kernel(x_hbm, ids_hbm, gates_hbm, wu_hbm, wd_hbm, y_ref, ids_ref, gates_ref, wu, wd, xg, back, hid, xs, posg, post, send_x, send_m, send_b, rf, rx, rm, rb, sw, sl, ready):
    me = lax.axis_index('ep')
    c = lax.rem(me, 2)
    x = lax.rem(me // 2, 2)
    y = me // 4

    def dev(yy, xx, cc):
        return yy * 4 + xx * 2 + cc

    partner = dev(y, x, 1 - c)
    first = dev(lax.rem(y + 1 - c, 2), lax.rem(x + c, 2), c)
    second = dev(lax.rem(y + c, 2), lax.rem(x + 1 - c, 2), c)
    def source(i, cc):
        lo, hi = lax.rem(i, 2), i // 2
        fy = lo * (1 - cc) + hi * cc
        fx = hi * (1 - cc) + lo * cc
        return dev(lax.rem(y + fy, 2), lax.rem(x + fx, 2), cc)

    own_load = pltpu.make_async_copy(x_hbm, xg.at[me], sl.at[0])
    own_load.start()
    barrier = pltpu.get_barrier_semaphore()
    for other in (partner, first):
        pl.semaphore_signal(barrier, inc=1, device_id={'ep': other}, device_id_type=MESH)
    ids_load = pltpu.make_async_copy(ids_hbm, ids_ref, sl.at[1])
    gates_load = pltpu.make_async_copy(gates_hbm, gates_ref, sl.at[2])
    ids_load.start()
    gates_load.start()
    def up_cols(t):
        return pl.ds(t * NU, min(NU, F - t * NU))

    def down_cols(n):
        return pl.ds(*DOWN[n])

    def msg_cols(m):
        return pl.ds(*MSG[m])

    def up_load(t):
        return pltpu.make_async_copy(wu_hbm.at[0, :, up_cols(t)], wu.at[:, up_cols(t)], sw.at[t])

    def down_load(n):
        cols = pl.ds(*((0, 1024), (1024, 1280))[n])
        return pltpu.make_async_copy(wd_hbm.at[0, :, cols], wd.at[:, cols], sw.at[NT + n])

    with jax.named_scope('own_load'):
        own_load.wait()
    for t in range(AHEAD):
        up_load(t).start()
    with jax.named_scope('barrier'):
        pl.semaphore_wait(barrier, 2)

    def half(s, p, recv_sem, to):
        rows = pl.ds(p * HALF, HALF)
        return remote(xg.at[s, rows], xg.at[s, rows], send_x, recv_sem, to)

    def block(s, to):
        return remote(xg.at[s], xg.at[s], send_x, rx.at[s], to)

    def arrived(s):
        block(s, partner).wait_recv()

    def meta_arrived(s):
        meta(s, partner).wait_recv()

    def meta(s, to):
        return remote(posg.at[s], posg.at[s], send_m, rm.at[s], to)

    def back_send(i, s, m):
        return remote(xg.at[source(i, 1 - c), pl.ds(s * CAP, CAP), msg_cols(m)], back.at[me, :, msg_cols(m)], send_b, rb.at[m], source(i, s))

    def back_partner(m):
        return remote(xg.at[partner, pl.ds(pl.multiple_of((1 - c) * CAP, CAP), CAP), msg_cols(m)], back.at[me, :, msg_cols(m)], send_b, rb.at[m], partner)

    def gather(i, s):
        s_id = source(i, s)
        where = posg[s_id, pl.ds(me, 1), :]
        rank_row = lax.broadcasted_iota(jnp.int32, (CAP, TOK), 0).astype(jnp.float32)
        pick = jnp.where(rank_row == where, 1.0, 0.0).astype(jnp.bfloat16)
        xs[s * CAP:(s + 1) * CAP, :] = jnp.dot(pick, xg[s_id], preferred_element_type=jnp.float32).astype(jnp.bfloat16)

    def up_tile(h, t):
        z = jnp.dot(xs[...], wu[:, up_cols(t)], preferred_element_type=jnp.float32)
        hid[h, :, up_cols(t)] = jax.nn.gelu(z, approximate=True).astype(jnp.bfloat16)

    def down_tile(h, i, n):
        xg[source(i, 1 - c), :, down_cols(n)] = jnp.dot(hid[h], wd[:, down_cols(n)], preferred_element_type=jnp.float32).astype(jnp.bfloat16)

    def own_down(n):
        down_tile(0, 0, n)
        for m in BLOCK_MSGS[n]:
            back_partner(m).start()
        back[me, :, down_cols(n)] = xg[partner, pl.ds(pl.multiple_of(c * CAP, CAP), CAP), down_cols(n)]

    half(me, 0, rf, first).start()
    block(me, partner).start()
    for t in range(AHEAD, 4):
        up_load(t).start()
    ids_load.wait()
    gates_load.wait()
    lane = lax.broadcasted_iota(jnp.int32, (TOK, TOK), 1)
    row = lax.broadcasted_iota(jnp.int32, (TOK, TOK), 0)
    expert_row = lax.broadcasted_iota(jnp.int32, (EXP, TOK), 0)
    hit = (ids_ref[0:1, :] == expert_row) | (ids_ref[1:2, :] == expert_row)
    upper = jnp.where(row < lane, 1.0, 0.0).astype(jnp.bfloat16)
    rank = jnp.dot(jnp.where(hit, 1.0, 0.0).astype(jnp.bfloat16), upper, preferred_element_type=jnp.float32)
    slots = jnp.where(hit, rank, -1.0)
    posg[me] = slots
    pad = jnp.zeros((TOK - EXP - 4, TOK), jnp.float32)
    post[...] = jnp.concatenate([slots, ids_ref[...].astype(jnp.float32), gates_ref[...], pad], axis=0).T
    for to in (first, partner):
        meta(me, to).start()
    half(me, 1, rx.at[me], first).start()
    near = source(1, c)
    with jax.named_scope('wait_partner'):
        meta_arrived(partner)
        arrived(partner)
    with jax.named_scope('up0'):
        gather(0, 0)
        gather(0, 1)
        for t in range(NT):
            up_load(t).wait()
            if t < 2:
                up_load(4 + t).start()
            if t == 2:
                down_load(0).start()
            if t == F_TILE:
                with jax.named_scope('wait_f0'):
                    meta_arrived(near)
                    half(near, 0, rf, partner).wait_recv()
                pl.semaphore_signal(ready, inc=1, device_id={'ep': partner}, device_id_type=MESH)
                pl.semaphore_wait(ready, 1)
                meta(me, second).start()
                for to in (second, partner):
                    meta(near, to).start()
                    half(near, 0, rx.at[near], to).start()
            if t == NT - 1:
                down_load(1).start()
                with jax.named_scope('wait_f1'):
                    half(near, 1, rx.at[near], partner).wait_recv()
                    for to in (second, partner):
                        half(near, 1, rx.at[near], to).start()
                    block(me, second).start()
            up_tile(0, t)

    def chunk(k, carry):
        i = jnp.where(k == 1, 1, 5 - k)
        with jax.named_scope('wait_chunk'):
            meta_arrived(source(i, 1 - c))
            arrived(source(i, 1 - c))
        with jax.named_scope('up'):
            gather(i, 0)
            gather(i, 1)
            for t in range(NT):
                up_tile(1, t)

        @pl.when(k == 1)
        def _():
            down_load(0).wait()

        for n in range(len(DOWN)):
            with jax.named_scope('down'):
                down_tile(1, i, n)

                @pl.when(k < 3)
                def _():
                    for m in BLOCK_MSGS[n]:
                        for s in range(2):
                            back_send(i, s, m).start()
            if n == 0:
                with jax.named_scope('wait_direct'):
                    @pl.when(k == 1)
                    def _():
                        down_load(1).wait()

                    @pl.when(k < 3)
                    def _():
                        after = source(4 - k, c)
                        meta_arrived(after)
                        arrived(after)
                        meta(after, partner).start()
                        block(after, partner).start()
        @pl.when(k == 3)
        def _():
            for m in range(NM):
                for s in range(2):
                    back_send(i, s, m).start()

        return carry

    lax.fori_loop(1, 4, chunk, 0)
    with jax.named_scope('own_down'):
        for n in range(len(DOWN)):
            own_down(n)

    cols8 = post[...]
    low = lane < CAP
    parts = []
    for k in range(EXP // 2):
        at = jnp.where(low, cols8[:, 2 * k:2 * k + 1], cols8[:, 2 * k + 1:2 * k + 2])
        here = at == (lane - jnp.where(low, 0, CAP)).astype(jnp.float32)
        parts.append((here, (2 * k + jnp.where(low, 0, 1)).astype(jnp.float32)))
    choice = [cols8[:, EXP + j:EXP + j + 1] for j in range(2)]
    picks = jnp.concatenate([jnp.concatenate([jnp.where(here & (expert == idj), 1.0, 0.0).astype(jnp.bfloat16) for here, expert in parts], axis=1) for idj in choice], axis=0)
    g0 = cols8[:, EXP + 2:EXP + 3]
    g1 = cols8[:, EXP + 3:EXP + 4]

    for m in range(NM):
        cols = msg_cols(m)
        with jax.named_scope('wait_back'):
            seven = back.at[pl.ds(0, EXP - 1), :, cols]
            remote(seven, seven, send_b, rb.at[m], partner).wait_recv()
        with jax.named_scope('combine'):
            rows = back[:, :, cols].reshape(EXP * CAP, MSG[m][1])
            got = jnp.dot(picks, rows, preferred_element_type=jnp.float32)
            y_ref[:, cols] = (g0 * got[:TOK] + g1 * got[TOK:]).astype(jnp.bfloat16)

    for sent, sem in ((xg, send_x), (posg, send_m), (back, send_b)):
        seven = sent.at[pl.ds(0, EXP - 1)]
        remote(seven, seven, sem, rf, partner).wait_send()


def solution(mesh):
    token_spec = P(('dp', 'ep'), None)
    expert_spec = P('ep', None, None)
    vmem = pl.BlockSpec(memory_space=pltpu.VMEM)
    anyspace = pl.BlockSpec(memory_space=pl.ANY)
    bf16, f32 = jnp.bfloat16, jnp.float32

    def local_layer(x_loc, ids_loc, gates_loc, w_up, w_down):
        return pl.pallas_call(
            moe_kernel,
            out_shape=pltpu.VMEM((TOK, D), bf16),
            in_specs=[anyspace] * 5,
            out_specs=vmem,
            scratch_shapes=[
                pltpu.VMEM((2, TOK), jnp.int32),
                pltpu.VMEM((2, TOK), f32),
                pltpu.VMEM((D, F), bf16),
                pltpu.VMEM((F, D), bf16),
                pltpu.VMEM((EXP, TOK, D), bf16),
                pltpu.VMEM((EXP, CAP, D), bf16),
                pltpu.VMEM((2, TOK, F), bf16),
                pltpu.VMEM((TOK, D), bf16),
                pltpu.VMEM((EXP, EXP, TOK), f32),
                pltpu.VMEM((TOK, TOK), f32),
                pltpu.SemaphoreType.DMA,
                pltpu.SemaphoreType.DMA,
                pltpu.SemaphoreType.DMA,
                pltpu.SemaphoreType.DMA,
                pltpu.SemaphoreType.DMA((EXP,)),
                pltpu.SemaphoreType.DMA((EXP,)),
                pltpu.SemaphoreType.DMA((NM,)),
                pltpu.SemaphoreType.DMA((NT + 2,)),
                pltpu.SemaphoreType.DMA((3,)),
                pltpu.SemaphoreType.REGULAR,
            ],
            compiler_params=pltpu.CompilerParams(vmem_limit_bytes=VMEM_LIMIT, collective_id=0, has_side_effects=True),
        )(x_loc, ids_loc.T, gates_loc.T, w_up, w_down)

    return jax.shard_map(local_layer, mesh=mesh, in_specs=(token_spec, token_spec, token_spec, expert_spec, expert_spec), out_specs=token_spec, check_vma=False)
```

```python
import functools

import jax
import jax.numpy as jnp
from jax import lax
from jax.experimental import pallas as pl
from jax.experimental.pallas import tpu as pltpu
from jax.sharding import PartitionSpec as P

MESH = pl.DeviceIdType.MESH
TOK = 128
CAP = 64
EXP = 8
D = 2304
F = 5760
NU = 1024
NT = -(-F // NU)
F_TILE = 3
AHEAD = 2
DOWN = ((0, 512), (512, 512), (1024, 1280))
MSG = ((0, 512), (512, 512), (1024, 640), (1664, 384), (2048, 256))
BLOCK_MSGS = ((0,), (1,), (2, 3, 4))
NM = len(MSG)
HALF = TOK // 2
VMEM_LIMIT = 66400000


def remote(src, dst, send_sem, recv_sem, dev):
    return pltpu.make_async_remote_copy(src_ref=src, dst_ref=dst, send_sem=send_sem, recv_sem=recv_sem, device_id={'ep': dev}, device_id_type=MESH)


def moe_kernel(x_hbm, ids_hbm, gates_hbm, wu_hbm, wd_hbm, y_ref, ids_ref, gates_ref, wu, wd, xg, back, hid, xs, posg, post, send_x, send_m, send_b, rf, rx, rm, rb, sw, sl, ready):
    me = lax.axis_index('ep')
    c = lax.rem(me, 2)
    x = lax.rem(me // 2, 2)
    y = me // 4

    def dev(yy, xx, cc):
        return yy * 4 + xx * 2 + cc

    partner = dev(y, x, 1 - c)
    first = dev(lax.rem(y + 1 - c, 2), lax.rem(x + c, 2), c)
    second = dev(lax.rem(y + c, 2), lax.rem(x + 1 - c, 2), c)
    def source(i, cc):
        lo, hi = lax.rem(i, 2), i // 2
        fy = lo * (1 - cc) + hi * cc
        fx = hi * (1 - cc) + lo * cc
        return dev(lax.rem(y + fy, 2), lax.rem(x + fx, 2), cc)

    own_loads = [pltpu.make_async_copy(x_hbm.at[pl.ds(p * HALF, HALF)], xg.at[me, pl.ds(p * HALF, HALF)], sl.at[3 * p]) for p in range(2)]
    for own_load in own_loads:
        own_load.start()
    barrier = pltpu.get_barrier_semaphore()
    for other in (partner, first):
        pl.semaphore_signal(barrier, inc=1, device_id={'ep': other}, device_id_type=MESH)
    ids_load = pltpu.make_async_copy(ids_hbm, ids_ref, sl.at[1])
    gates_load = pltpu.make_async_copy(gates_hbm, gates_ref, sl.at[2])
    ids_load.start()
    gates_load.start()
    def up_cols(t):
        return pl.ds(t * NU, min(NU, F - t * NU))

    def down_cols(n):
        return pl.ds(*DOWN[n])

    def msg_cols(m):
        return pl.ds(*MSG[m])

    def up_load(t):
        return pltpu.make_async_copy(wu_hbm.at[0, :, up_cols(t)], wu.at[:, up_cols(t)], sw.at[t])

    def down_load(n):
        cols = pl.ds(*((0, 1024), (1024, 1280))[n])
        return pltpu.make_async_copy(wd_hbm.at[0, :, cols], wd.at[:, cols], sw.at[NT + n])

    with jax.named_scope('own_load'):
        own_loads[0].wait()
    for t in range(AHEAD):
        up_load(t).start()
    with jax.named_scope('barrier'):
        pl.semaphore_wait(barrier, 2)

    def half(s, p, recv_sem, to):
        rows = pl.ds(p * HALF, HALF)
        return remote(xg.at[s, rows], xg.at[s, rows], send_x, recv_sem, to)

    def block(s, to):
        return remote(xg.at[s], xg.at[s], send_x, rx.at[s], to)

    def arrived(s):
        block(s, partner).wait_recv()

    def meta_arrived(s):
        meta(s, partner).wait_recv()

    def meta(s, to):
        return remote(posg.at[s], posg.at[s], send_m, rm.at[s], to)

    def back_send(i, s, m):
        return remote(xg.at[source(i, 1 - c), pl.ds(s * CAP, CAP), msg_cols(m)], back.at[me, :, msg_cols(m)], send_b, rb.at[m], source(i, s))

    def back_partner(m):
        return remote(xg.at[partner, pl.ds(pl.multiple_of((1 - c) * CAP, CAP), CAP), msg_cols(m)], back.at[me, :, msg_cols(m)], send_b, rb.at[m], partner)

    def gather(i, s):
        s_id = source(i, s)
        where = posg[s_id, pl.ds(me, 1), :]
        rank_row = lax.broadcasted_iota(jnp.int32, (CAP, TOK), 0).astype(jnp.float32)
        pick = jnp.where(rank_row == where, 1.0, 0.0).astype(jnp.bfloat16)
        xs[s * CAP:(s + 1) * CAP, :] = jnp.dot(pick, xg[s_id], preferred_element_type=jnp.float32).astype(jnp.bfloat16)

    def up_tile(h, t):
        z = jnp.dot(xs[...], wu[:, up_cols(t)], preferred_element_type=jnp.float32)
        hid[h, :, up_cols(t)] = jax.nn.gelu(z, approximate=True).astype(jnp.bfloat16)

    def down_tile(h, i, n):
        xg[source(i, 1 - c), :, down_cols(n)] = jnp.dot(hid[h], wd[:, down_cols(n)], preferred_element_type=jnp.float32).astype(jnp.bfloat16)

    def own_down(n):
        down_tile(0, 0, n)
        for m in BLOCK_MSGS[n]:
            back_partner(m).start()
        back[me, :, down_cols(n)] = xg[partner, pl.ds(pl.multiple_of(c * CAP, CAP), CAP), down_cols(n)]

    half(me, 0, rf, first).start()
    own_loads[1].wait()
    block(me, partner).start()
    for t in range(AHEAD, 4):
        up_load(t).start()
    ids_load.wait()
    gates_load.wait()
    lane = lax.broadcasted_iota(jnp.int32, (TOK, TOK), 1)
    row = lax.broadcasted_iota(jnp.int32, (TOK, TOK), 0)
    expert_row = lax.broadcasted_iota(jnp.int32, (EXP, TOK), 0)
    hit = (ids_ref[0:1, :] == expert_row) | (ids_ref[1:2, :] == expert_row)
    upper = jnp.where(row < lane, 1.0, 0.0).astype(jnp.bfloat16)
    rank = jnp.dot(jnp.where(hit, 1.0, 0.0).astype(jnp.bfloat16), upper, preferred_element_type=jnp.float32)
    slots = jnp.where(hit, rank, -1.0)
    posg[me] = slots
    pad = jnp.zeros((TOK - EXP - 4, TOK), jnp.float32)
    post[...] = jnp.concatenate([slots, ids_ref[...].astype(jnp.float32), gates_ref[...], pad], axis=0).T
    for to in (first, partner):
        meta(me, to).start()
    half(me, 1, rx.at[me], first).start()
    near = source(1, c)
    with jax.named_scope('wait_partner'):
        meta_arrived(partner)
        arrived(partner)
    with jax.named_scope('up0'):
        gather(0, 0)
        gather(0, 1)
        for t in range(NT):
            up_load(t).wait()
            if t < 2:
                up_load(4 + t).start()
            if t == 2:
                down_load(0).start()
            if t == F_TILE:
                with jax.named_scope('wait_f0'):
                    meta_arrived(near)
                    half(near, 0, rf, partner).wait_recv()
                pl.semaphore_signal(ready, inc=1, device_id={'ep': partner}, device_id_type=MESH)
                pl.semaphore_wait(ready, 1)
                meta(me, second).start()
                for to in (second, partner):
                    meta(near, to).start()
                    half(near, 0, rx.at[near], to).start()
            if t == NT - 1:
                down_load(1).start()
                with jax.named_scope('wait_f1'):
                    half(near, 1, rx.at[near], partner).wait_recv()
                    for to in (second, partner):
                        half(near, 1, rx.at[near], to).start()
                    block(me, second).start()
            up_tile(0, t)

    def chunk(k, carry):
        i = jnp.where(k == 1, 1, 5 - k)
        with jax.named_scope('wait_chunk'):
            meta_arrived(source(i, 1 - c))
            arrived(source(i, 1 - c))
        with jax.named_scope('up'):
            gather(i, 0)
            gather(i, 1)
            for t in range(NT):
                up_tile(1, t)

        @pl.when(k == 1)
        def _():
            down_load(0).wait()

        for n in range(len(DOWN)):
            with jax.named_scope('down'):
                down_tile(1, i, n)

                @pl.when(k < 3)
                def _():
                    for m in BLOCK_MSGS[n]:
                        for s in range(2):
                            back_send(i, s, m).start()
            if n == 0:
                with jax.named_scope('wait_direct'):
                    @pl.when(k == 1)
                    def _():
                        down_load(1).wait()

                    @pl.when(k < 3)
                    def _():
                        after = source(4 - k, c)
                        meta_arrived(after)
                        arrived(after)
                        meta(after, partner).start()
                        block(after, partner).start()
        @pl.when(k == 3)
        def _():
            for m in range(NM):
                for s in range(2):
                    back_send(i, s, m).start()

        return carry

    lax.fori_loop(1, 4, chunk, 0)
    with jax.named_scope('own_down'):
        for n in range(len(DOWN)):
            own_down(n)

    cols8 = post[...]
    low = lane < CAP
    parts = []
    for k in range(EXP // 2):
        at = jnp.where(low, cols8[:, 2 * k:2 * k + 1], cols8[:, 2 * k + 1:2 * k + 2])
        here = at == (lane - jnp.where(low, 0, CAP)).astype(jnp.float32)
        parts.append((here, (2 * k + jnp.where(low, 0, 1)).astype(jnp.float32)))
    choice = [cols8[:, EXP + j:EXP + j + 1] for j in range(2)]
    picks = jnp.concatenate([jnp.concatenate([jnp.where(here & (expert == idj), 1.0, 0.0).astype(jnp.bfloat16) for here, expert in parts], axis=1) for idj in choice], axis=0)
    g0 = cols8[:, EXP + 2:EXP + 3]
    g1 = cols8[:, EXP + 3:EXP + 4]

    for m in range(NM):
        cols = msg_cols(m)
        with jax.named_scope('wait_back'):
            seven = back.at[pl.ds(0, EXP - 1), :, cols]
            remote(seven, seven, send_b, rb.at[m], partner).wait_recv()
        with jax.named_scope('combine'):
            rows = back[:, :, cols].reshape(EXP * CAP, MSG[m][1])
            got = jnp.dot(picks, rows, preferred_element_type=jnp.float32)
            y_ref[:, cols] = (g0 * got[:TOK] + g1 * got[TOK:]).astype(jnp.bfloat16)

    for sent, sem in ((xg, send_x), (posg, send_m), (back, send_b)):
        seven = sent.at[pl.ds(0, EXP - 1)]
        remote(seven, seven, sem, rf, partner).wait_send()


def solution(mesh):
    token_spec = P(('dp', 'ep'), None)
    expert_spec = P('ep', None, None)
    vmem = pl.BlockSpec(memory_space=pltpu.VMEM)
    anyspace = pl.BlockSpec(memory_space=pl.ANY)
    bf16, f32 = jnp.bfloat16, jnp.float32

    def local_layer(x_loc, ids_loc, gates_loc, w_up, w_down):
        return pl.pallas_call(
            moe_kernel,
            out_shape=pltpu.VMEM((TOK, D), bf16),
            in_specs=[anyspace] * 5,
            out_specs=vmem,
            scratch_shapes=[
                pltpu.VMEM((2, TOK), jnp.int32),
                pltpu.VMEM((2, TOK), f32),
                pltpu.VMEM((D, F), bf16),
                pltpu.VMEM((F, D), bf16),
                pltpu.VMEM((EXP, TOK, D), bf16),
                pltpu.VMEM((EXP, CAP, D), bf16),
                pltpu.VMEM((2, TOK, F), bf16),
                pltpu.VMEM((TOK, D), bf16),
                pltpu.VMEM((EXP, EXP, TOK), f32),
                pltpu.VMEM((TOK, TOK), f32),
                pltpu.SemaphoreType.DMA,
                pltpu.SemaphoreType.DMA,
                pltpu.SemaphoreType.DMA,
                pltpu.SemaphoreType.DMA,
                pltpu.SemaphoreType.DMA((EXP,)),
                pltpu.SemaphoreType.DMA((EXP,)),
                pltpu.SemaphoreType.DMA((NM,)),
                pltpu.SemaphoreType.DMA((NT + 2,)),
                pltpu.SemaphoreType.DMA((4,)),
                pltpu.SemaphoreType.REGULAR,
            ],
            compiler_params=pltpu.CompilerParams(vmem_limit_bytes=VMEM_LIMIT, collective_id=0, has_side_effects=True),
        )(x_loc, ids_loc.T, gates_loc.T, w_up, w_down)

    return jax.shard_map(local_layer, mesh=mesh, in_specs=(token_spec, token_spec, token_spec, expert_spec, expert_spec), out_specs=token_spec, check_vma=False)
```

```python
import functools

import jax
import jax.numpy as jnp
from jax import lax
from jax.experimental import pallas as pl
from jax.experimental.pallas import tpu as pltpu
from jax.sharding import PartitionSpec as P

MESH = pl.DeviceIdType.MESH
TOK = 128
CAP = 64
EXP = 8
D = 2304
F = 5760
NU = 1024
NT = -(-F // NU)
F_TILE = 3
AHEAD = 2
DOWN = ((0, 512), (512, 512), (1024, 1280))
MSG = ((0, 512), (512, 512), (1024, 640), (1664, 256), (1920, 256), (2176, 128))
BLOCK_MSGS = ((0,), (1,), (2, 3, 4, 5))
NM = len(MSG)
HALF = TOK // 2
VMEM_LIMIT = 66400000


def remote(src, dst, send_sem, recv_sem, dev):
    return pltpu.make_async_remote_copy(src_ref=src, dst_ref=dst, send_sem=send_sem, recv_sem=recv_sem, device_id={'ep': dev}, device_id_type=MESH)


def moe_kernel(x_hbm, ids_hbm, gates_hbm, wu_hbm, wd_hbm, y_ref, ids_ref, gates_ref, wu, wd, xg, back, hid, xs, posg, post, send_x, send_m, send_b, rf, rx, rm, rb, sw, sl, ready):
    me = lax.axis_index('ep')
    c = lax.rem(me, 2)
    x = lax.rem(me // 2, 2)
    y = me // 4

    def dev(yy, xx, cc):
        return yy * 4 + xx * 2 + cc

    partner = dev(y, x, 1 - c)
    first = dev(lax.rem(y + 1 - c, 2), lax.rem(x + c, 2), c)
    second = dev(lax.rem(y + c, 2), lax.rem(x + 1 - c, 2), c)
    def source(i, cc):
        lo, hi = lax.rem(i, 2), i // 2
        fy = lo * (1 - cc) + hi * cc
        fx = hi * (1 - cc) + lo * cc
        return dev(lax.rem(y + fy, 2), lax.rem(x + fx, 2), cc)

    own_loads = [pltpu.make_async_copy(x_hbm.at[pl.ds(p * HALF, HALF)], xg.at[me, pl.ds(p * HALF, HALF)], sl.at[3 * p]) for p in range(2)]
    for own_load in own_loads:
        own_load.start()
    barrier = pltpu.get_barrier_semaphore()
    for other in (partner, first):
        pl.semaphore_signal(barrier, inc=1, device_id={'ep': other}, device_id_type=MESH)
    ids_load = pltpu.make_async_copy(ids_hbm, ids_ref, sl.at[1])
    gates_load = pltpu.make_async_copy(gates_hbm, gates_ref, sl.at[2])
    ids_load.start()
    gates_load.start()
    def up_cols(t):
        return pl.ds(t * NU, min(NU, F - t * NU))

    def down_cols(n):
        return pl.ds(*DOWN[n])

    def msg_cols(m):
        return pl.ds(*MSG[m])

    def up_load(t):
        return pltpu.make_async_copy(wu_hbm.at[0, :, up_cols(t)], wu.at[:, up_cols(t)], sw.at[t])

    def down_load(n):
        cols = pl.ds(*((0, 1024), (1024, 1280))[n])
        return pltpu.make_async_copy(wd_hbm.at[0, :, cols], wd.at[:, cols], sw.at[NT + n])

    with jax.named_scope('own_load'):
        own_loads[0].wait()
    for t in range(AHEAD):
        up_load(t).start()
    with jax.named_scope('barrier'):
        pl.semaphore_wait(barrier, 2)

    def half(s, p, recv_sem, to):
        rows = pl.ds(p * HALF, HALF)
        return remote(xg.at[s, rows], xg.at[s, rows], send_x, recv_sem, to)

    def block(s, to):
        return remote(xg.at[s], xg.at[s], send_x, rx.at[s], to)

    def arrived(s):
        block(s, partner).wait_recv()

    def meta_arrived(s):
        meta(s, partner).wait_recv()

    def meta(s, to):
        return remote(posg.at[s], posg.at[s], send_m, rm.at[s], to)

    def back_send(i, s, m):
        return remote(xg.at[source(i, 1 - c), pl.ds(s * CAP, CAP), msg_cols(m)], back.at[me, :, msg_cols(m)], send_b, rb.at[m], source(i, s))

    def back_partner(m):
        return remote(xg.at[partner, pl.ds(pl.multiple_of((1 - c) * CAP, CAP), CAP), msg_cols(m)], back.at[me, :, msg_cols(m)], send_b, rb.at[m], partner)

    def gather(i, s):
        s_id = source(i, s)
        where = posg[s_id, pl.ds(me, 1), :]
        rank_row = lax.broadcasted_iota(jnp.int32, (CAP, TOK), 0).astype(jnp.float32)
        pick = jnp.where(rank_row == where, 1.0, 0.0).astype(jnp.bfloat16)
        xs[s * CAP:(s + 1) * CAP, :] = jnp.dot(pick, xg[s_id], preferred_element_type=jnp.float32).astype(jnp.bfloat16)

    def up_tile(h, t):
        z = jnp.dot(xs[...], wu[:, up_cols(t)], preferred_element_type=jnp.float32)
        hid[h, :, up_cols(t)] = jax.nn.gelu(z, approximate=True).astype(jnp.bfloat16)

    def down_tile(h, i, n):
        xg[source(i, 1 - c), :, down_cols(n)] = jnp.dot(hid[h], wd[:, down_cols(n)], preferred_element_type=jnp.float32).astype(jnp.bfloat16)

    def own_down(n):
        down_tile(0, 0, n)
        for m in BLOCK_MSGS[n]:
            back_partner(m).start()
        back[me, :, down_cols(n)] = xg[partner, pl.ds(pl.multiple_of(c * CAP, CAP), CAP), down_cols(n)]

    half(me, 0, rf, first).start()
    own_loads[1].wait()
    block(me, partner).start()
    for t in range(AHEAD, 4):
        up_load(t).start()
    ids_load.wait()
    gates_load.wait()
    lane = lax.broadcasted_iota(jnp.int32, (TOK, TOK), 1)
    row = lax.broadcasted_iota(jnp.int32, (TOK, TOK), 0)
    expert_row = lax.broadcasted_iota(jnp.int32, (EXP, TOK), 0)
    hit = (ids_ref[0:1, :] == expert_row) | (ids_ref[1:2, :] == expert_row)
    upper = jnp.where(row < lane, 1.0, 0.0).astype(jnp.bfloat16)
    rank = jnp.dot(jnp.where(hit, 1.0, 0.0).astype(jnp.bfloat16), upper, preferred_element_type=jnp.float32)
    slots = jnp.where(hit, rank, -1.0)
    posg[me] = slots
    pad = jnp.zeros((TOK - EXP - 4, TOK), jnp.float32)
    post[...] = jnp.concatenate([slots, ids_ref[...].astype(jnp.float32), gates_ref[...], pad], axis=0).T
    for to in (first, partner):
        meta(me, to).start()
    half(me, 1, rx.at[me], first).start()
    near = source(1, c)
    with jax.named_scope('wait_partner'):
        meta_arrived(partner)
        arrived(partner)
    with jax.named_scope('up0'):
        gather(0, 0)
        gather(0, 1)
        for t in range(NT):
            up_load(t).wait()
            if t < 2:
                up_load(4 + t).start()
            if t == 2:
                down_load(0).start()
            if t == F_TILE:
                with jax.named_scope('wait_f0'):
                    meta_arrived(near)
                    half(near, 0, rf, partner).wait_recv()
                pl.semaphore_signal(ready, inc=1, device_id={'ep': partner}, device_id_type=MESH)
                pl.semaphore_wait(ready, 1)
                meta(me, second).start()
                for to in (second, partner):
                    meta(near, to).start()
                    half(near, 0, rx.at[near], to).start()
            if t == NT - 1:
                down_load(1).start()
                with jax.named_scope('wait_f1'):
                    half(near, 1, rx.at[near], partner).wait_recv()
                    for to in (second, partner):
                        half(near, 1, rx.at[near], to).start()
                    block(me, second).start()
            up_tile(0, t)

    def chunk(k, carry):
        i = jnp.where(k == 1, 1, 5 - k)
        with jax.named_scope('wait_chunk'):
            meta_arrived(source(i, 1 - c))
            arrived(source(i, 1 - c))
        with jax.named_scope('up'):
            gather(i, 0)
            gather(i, 1)
            for t in range(NT):
                up_tile(1, t)

        @pl.when(k == 1)
        def _():
            down_load(0).wait()

        for n in range(len(DOWN)):
            with jax.named_scope('down'):
                down_tile(1, i, n)

                @pl.when(k < 3)
                def _():
                    for m in BLOCK_MSGS[n]:
                        for s in range(2):
                            back_send(i, s, m).start()
            if n == 0:
                with jax.named_scope('wait_direct'):
                    @pl.when(k == 1)
                    def _():
                        down_load(1).wait()

                    @pl.when(k < 3)
                    def _():
                        after = source(4 - k, c)
                        meta_arrived(after)
                        arrived(after)
                        meta(after, partner).start()
                        block(after, partner).start()
        @pl.when(k == 3)
        def _():
            for m in range(NM):
                for s in range(2):
                    back_send(i, s, m).start()

        return carry

    lax.fori_loop(1, 4, chunk, 0)
    with jax.named_scope('own_down'):
        for n in range(len(DOWN)):
            own_down(n)

    cols8 = post[...]
    low = lane < CAP
    parts = []
    for k in range(EXP // 2):
        at = jnp.where(low, cols8[:, 2 * k:2 * k + 1], cols8[:, 2 * k + 1:2 * k + 2])
        here = at == (lane - jnp.where(low, 0, CAP)).astype(jnp.float32)
        parts.append((here, (2 * k + jnp.where(low, 0, 1)).astype(jnp.float32)))
    choice = [cols8[:, EXP + j:EXP + j + 1] for j in range(2)]
    picks = jnp.concatenate([jnp.concatenate([jnp.where(here & (expert == idj), 1.0, 0.0).astype(jnp.bfloat16) for here, expert in parts], axis=1) for idj in choice], axis=0)
    g0 = cols8[:, EXP + 2:EXP + 3]
    g1 = cols8[:, EXP + 3:EXP + 4]

    for m in range(NM):
        cols = msg_cols(m)
        with jax.named_scope('wait_back'):
            seven = back.at[pl.ds(0, EXP - 1), :, cols]
            remote(seven, seven, send_b, rb.at[m], partner).wait_recv()
        with jax.named_scope('combine'):
            rows = back[:, :, cols].reshape(EXP * CAP, MSG[m][1])
            got = jnp.dot(picks, rows, preferred_element_type=jnp.float32)
            y_ref[:, cols] = (g0 * got[:TOK] + g1 * got[TOK:]).astype(jnp.bfloat16)

    for sent, sem in ((xg, send_x), (posg, send_m), (back, send_b)):
        seven = sent.at[pl.ds(0, EXP - 1)]
        remote(seven, seven, sem, rf, partner).wait_send()


def solution(mesh):
    token_spec = P(('dp', 'ep'), None)
    expert_spec = P('ep', None, None)
    vmem = pl.BlockSpec(memory_space=pltpu.VMEM)
    anyspace = pl.BlockSpec(memory_space=pl.ANY)
    bf16, f32 = jnp.bfloat16, jnp.float32

    def local_layer(x_loc, ids_loc, gates_loc, w_up, w_down):
        return pl.pallas_call(
            moe_kernel,
            out_shape=pltpu.VMEM((TOK, D), bf16),
            in_specs=[anyspace] * 5,
            out_specs=vmem,
            scratch_shapes=[
                pltpu.VMEM((2, TOK), jnp.int32),
                pltpu.VMEM((2, TOK), f32),
                pltpu.VMEM((D, F), bf16),
                pltpu.VMEM((F, D), bf16),
                pltpu.VMEM((EXP, TOK, D), bf16),
                pltpu.VMEM((EXP, CAP, D), bf16),
                pltpu.VMEM((2, TOK, F), bf16),
                pltpu.VMEM((TOK, D), bf16),
                pltpu.VMEM((EXP, EXP, TOK), f32),
                pltpu.VMEM((TOK, TOK), f32),
                pltpu.SemaphoreType.DMA,
                pltpu.SemaphoreType.DMA,
                pltpu.SemaphoreType.DMA,
                pltpu.SemaphoreType.DMA,
                pltpu.SemaphoreType.DMA((EXP,)),
                pltpu.SemaphoreType.DMA((EXP,)),
                pltpu.SemaphoreType.DMA((NM,)),
                pltpu.SemaphoreType.DMA((NT + 2,)),
                pltpu.SemaphoreType.DMA((4,)),
                pltpu.SemaphoreType.REGULAR,
            ],
            compiler_params=pltpu.CompilerParams(vmem_limit_bytes=VMEM_LIMIT, collective_id=0, has_side_effects=True),
        )(x_loc, ids_loc.T, gates_loc.T, w_up, w_down)

    return jax.shard_map(local_layer, mesh=mesh, in_specs=(token_spec, token_spec, token_spec, expert_spec, expert_spec), out_specs=token_spec, check_vma=False)
```
